32 devices in a mesh: dp: 1 (over z), cp: 4 (over y), tp: 8 (over x, core).
Axes of the slice: x: 4, y: 4, z: 1, core: 2. Of those that a mesh axis runs over, the one named last changes fastest.
The devices are a block of a 4x4x8 slice.
Arguments:
- x: bfloat16 [1, 8192, 5120], P('dp', ('cp', 'tp'))
- g_attn: bfloat16 [5120], replicated
- w_q: bfloat16 [5120, 32, 128], P(None, 'tp')
- w_k: bfloat16 [5120, 8, 128], P(None, 'tp')
- w_v: bfloat16 [5120, 8, 128], P(None, 'tp')
- w_o: bfloat16 [32, 128, 5120], P('tp')
- g_mlp: bfloat16 [5120], replicated
- w_gate: bfloat16 [5120, 14336], P(None, 'tp')
- w_up: bfloat16 [5120, 14336], P(None, 'tp')
- w_down: bfloat16 [14336, 5120], P('tp')
Outputs:
- output: bfloat16 [1, 8192, 5120], P('dp', ('cp', 'tp'))
All inputs are finite; a program needn't handle non-finite values.
Results may differ from the reference program's by a relative error of at most 0.02.
Values are sent between devices in bfloat16 or wider.
A program may use at most 768 MiB of HBM per device.

```python
import math
import jax
import jax.numpy as jnp
from jax import lax

SEQ_LEN = 8192
MODEL_DIM = 5120
N_HEADS = 32
N_KV_HEADS = 8
HEAD_DIM = 128
FFN_DIM = 14336
CP_SIZE = 4
Q_BLOCK = 128
NORM_EPS = 1e-5
ROPE_THETA = 500000.0


def stored_positions(row_ids):
    piece_len = SEQ_LEN // (2 * CP_SIZE)
    owner_cp = row_ids // (2 * piece_len)
    within = row_ids % (2 * piece_len)
    return jnp.where(within < piece_len, owner_cp * piece_len + within,
                     (2 * CP_SIZE - 1 - owner_cp) * piece_len + within - piece_len)


def rms_norm(rows_in, gain_vec):
    rows_f32 = rows_in.astype(jnp.float32)
    mean_sq = jnp.mean(rows_f32 * rows_f32, axis=-1, keepdims=True)
    return (rows_f32 * lax.rsqrt(mean_sq + NORM_EPS) * gain_vec.astype(jnp.float32)).astype(jnp.bfloat16)


def apply_rope(heads_in, positions):
    half_dim = HEAD_DIM // 2
    inv_freq = ROPE_THETA ** (-2.0 * jnp.arange(half_dim, dtype=jnp.float32) / HEAD_DIM)
    angles = positions.astype(jnp.float32)[:, None] * inv_freq[None, :]
    angles = jnp.concatenate([angles, angles], axis=-1)[:, None, :]
    heads_f32 = heads_in.astype(jnp.float32)
    rotated = jnp.concatenate([-heads_f32[..., half_dim:], heads_f32[..., :half_dim]], axis=-1)
    return (heads_f32 * jnp.cos(angles) + rotated * jnp.sin(angles)).astype(jnp.bfloat16)


def draw_weight(key_in, weight_shape, std_dev):
    return (std_dev * jax.random.normal(key_in, weight_shape, jnp.float32)).astype(jnp.bfloat16)


def setup_inputs(seed: int = 0, part: int = 0) -> dict:
    key_list = jax.random.split(jax.random.key(seed), 10)
    qk_std = math.log(SEQ_LEN / 32.0) ** 0.25 / math.sqrt(MODEL_DIM)
    x = 0.5 * jax.random.normal(jax.random.fold_in(key_list[0], part), (1, SEQ_LEN, MODEL_DIM), jnp.float32)
    return {
        'x': x.astype(jnp.bfloat16),
        'g_attn': (0.5 + jax.random.uniform(key_list[1], (MODEL_DIM,), jnp.float32)).astype(jnp.bfloat16),
        'w_q': draw_weight(key_list[2], (MODEL_DIM, N_HEADS, HEAD_DIM), qk_std),
        'w_k': draw_weight(key_list[3], (MODEL_DIM, N_KV_HEADS, HEAD_DIM), qk_std),
        'w_v': draw_weight(key_list[4], (MODEL_DIM, N_KV_HEADS, HEAD_DIM), MODEL_DIM ** -0.5),
        'w_o': draw_weight(key_list[5], (N_HEADS, HEAD_DIM, MODEL_DIM), 2.0 * (N_HEADS * HEAD_DIM) ** -0.5),
        'g_mlp': (0.5 + jax.random.uniform(key_list[6], (MODEL_DIM,), jnp.float32)).astype(jnp.bfloat16),
        'w_gate': draw_weight(key_list[7], (MODEL_DIM, FFN_DIM), MODEL_DIM ** -0.5),
        'w_up': draw_weight(key_list[8], (MODEL_DIM, FFN_DIM), MODEL_DIM ** -0.5),
        'w_down': draw_weight(key_list[9], (FFN_DIM, MODEL_DIM), FFN_DIM ** -0.5),
    }


def reference(x, g_attn, w_q, w_k, w_v, w_o, g_mlp, w_gate, w_up, w_down):
    group_size = N_HEADS // N_KV_HEADS
    n_blocks = SEQ_LEN // Q_BLOCK
    positions = stored_positions(jnp.arange(SEQ_LEN, dtype=jnp.int32))
    x_rows = x[0]
    normed = rms_norm(x_rows, g_attn)
    q_all = jnp.dot(normed, w_q.reshape(MODEL_DIM, N_HEADS * HEAD_DIM), preferred_element_type=jnp.float32).astype(jnp.bfloat16)
    k_all = jnp.dot(normed, w_k.reshape(MODEL_DIM, N_KV_HEADS * HEAD_DIM), preferred_element_type=jnp.float32).astype(jnp.bfloat16)
    v_all = jnp.dot(normed, w_v.reshape(MODEL_DIM, N_KV_HEADS * HEAD_DIM), preferred_element_type=jnp.float32).astype(jnp.bfloat16)
    q_all = apply_rope(q_all.reshape(SEQ_LEN, N_HEADS, HEAD_DIM), positions)
    k_all = apply_rope(k_all.reshape(SEQ_LEN, N_KV_HEADS, HEAD_DIM), positions).astype(jnp.float32)
    v_all = v_all.reshape(SEQ_LEN, N_KV_HEADS, HEAD_DIM).astype(jnp.float32)
    w_o_flat = w_o.reshape(N_HEADS * HEAD_DIM, MODEL_DIM)
    score_scale = HEAD_DIM ** -0.5

    def one_block(block_in):
        q_blk, pos_blk, x_blk = block_in
        q_grp = q_blk.reshape(Q_BLOCK, N_KV_HEADS, group_size, HEAD_DIM).astype(jnp.float32)
        scores = jnp.einsum('qgrd,kgd->gqrk', q_grp, k_all) * score_scale
        visible = pos_blk[None, :, None, None] >= positions[None, None, None, :]
        scores = jnp.where(visible, scores, -1e30)
        weights = jnp.exp(scores - jnp.max(scores, axis=-1, keepdims=True))
        row_sum = jnp.sum(weights, axis=-1, keepdims=True)
        mixed_vals = jnp.einsum('gqrk,kgd->gqrd', weights.astype(jnp.bfloat16).astype(jnp.float32), v_all) / row_sum
        attn_rows = jnp.transpose(mixed_vals, (1, 0, 2, 3)).astype(jnp.bfloat16).reshape(Q_BLOCK, N_HEADS * HEAD_DIM)
        attn_proj = jnp.dot(attn_rows, w_o_flat, preferred_element_type=jnp.float32).astype(jnp.bfloat16)
        resid_rows = (x_blk.astype(jnp.float32) + attn_proj.astype(jnp.float32)).astype(jnp.bfloat16)
        normed_mlp = rms_norm(resid_rows, g_mlp)
        gate_proj = jnp.dot(normed_mlp, w_gate, preferred_element_type=jnp.float32)
        up_proj = jnp.dot(normed_mlp, w_up, preferred_element_type=jnp.float32)
        hidden = (jax.nn.silu(gate_proj) * up_proj).astype(jnp.bfloat16)
        down_proj = jnp.dot(hidden, w_down, preferred_element_type=jnp.float32).astype(jnp.bfloat16)
        return (resid_rows.astype(jnp.float32) + down_proj.astype(jnp.float32)).astype(jnp.bfloat16)

    blocks = lax.map(one_block, (q_all.reshape(n_blocks, Q_BLOCK, N_HEADS, HEAD_DIM),
                                 positions.reshape(n_blocks, Q_BLOCK),
                                 x_rows.reshape(n_blocks, Q_BLOCK, MODEL_DIM)))
    return blocks.reshape(1, SEQ_LEN, MODEL_DIM)
```

```python
import functools

import jax
import jax.numpy as jnp
from jax import lax
from jax.experimental import pallas as pl
from jax.experimental.pallas import tpu as pltpu
from jax.sharding import PartitionSpec as P

NORM_EPS = 1e-5
ROPE_THETA = 500000.0
MESH = pl.DeviceIdType.MESH
VMEM_LIMIT = 67_000_000
LOG2E = 1.4426950408889634
VM = pl.BlockSpec(memory_space=pltpu.VMEM)
HBM = pl.BlockSpec(memory_space=pl.ANY)


def params(ident):
    return pltpu.CompilerParams(collective_id=ident, has_side_effects=True, vmem_limit_bytes=VMEM_LIMIT)


def remote(src, dst, send_sem, recv_sem, **where):
    return pltpu.make_async_remote_copy(
        src_ref=src, dst_ref=dst, send_sem=send_sem, recv_sem=recv_sem,
        device_id=where, device_id_type=MESH)


def ring(n_tp):
    n_chips = n_tp // 2
    me = lax.axis_index('tp')
    chip, core = me // 2, me % 2
    other = chip * 2 + (1 - core)
    right = ((chip + 1) % n_chips) * 2 + core
    left = ((chip + n_chips - 1) % n_chips) * 2 + core
    return me, chip, core, other, right, left


def greet(barrier, partners):
    for where in partners:
        pl.semaphore_signal(barrier, inc=1, device_id=where, device_id_type=MESH)
    pl.semaphore_wait(barrier, len(partners))


def unit_place(o):
    far = (7 - o) // 6
    near = o // 6
    offset = 2 * far + (1 - far - near) * (1 - 2 * (o % 2))
    half = (o % 2 + ((o // 2) % 2) * (1 - o // 4)) % 2
    return offset, half


def pair_of(b):
    mid = ((b + 1) // 2) % 2
    return mid * b + (1 - mid) * (3 - b)


class Chips:
    def __init__(self, n_tp):
        self.n_chips = n_tp // 2
        self.me, self.chip, self.core, self.other, self.right, self.left = ring(n_tp)

    def place(self, o, flip):
        offset, half = unit_place(o)
        return ((self.chip + offset + self.n_chips) % self.n_chips) * 2 + (self.core + flip) % 2, half


class Gather(Chips):
    def __init__(self, n_tp, src, gath, send_sem, recv_sem):
        super().__init__(n_tp)
        self.src, self.gath, self.send_sem, self.recv_sem = src, gath, send_sem, recv_sem

    @staticmethod
    def sems():
        return [pltpu.SemaphoreType.DMA((2, 4, 4)), pltpu.SemaphoreType.DMA((4, 4))]

    def part(self, b, e):
        return self.gath.at[b, pl.ds(e * 128, 128)]

    def copy(self, src, b, e, dst, lane=1):
        return remote(src, self.part(b, e), self.send_sem.at[lane, b, e], self.recv_sem.at[b, e], tp=dst)

    def start(self, half):
        self.copy(self.src(half), 1, 1 - half, (self.right, self.left)[half]).start()
        self.copy(self.src(half), 0, 2 + half, self.other, 0).start()
        if half:
            self.copy(self.src(1), 2, 1, self.right).start()
            self.copy(self.src(0), 2, 0, self.left).start()

    def take(self, b, flip):
        for i in range(2):
            e = 2 * flip + i
            here = self.part(b, e)
            if flip or b:
                self.copy(here, b, e, self.other).wait_recv()
            if b and not flip:
                if b == 1:
                    self.copy(here, 3, 1 - i, (self.left, self.right)[i]).start()
                self.copy(here, b, 2 + i, self.other, 0).start()

    def finish(self):
        for i in range(2):
            for b in range(4):
                self.copy(self.src(0), b, 2 + i, self.other, 0).wait_send()
                if b:
                    self.copy(self.src(0), b, i, self.other).wait_send()


def chunk(j, size):
    return pl.ds(j * size if isinstance(j, int) else pl.multiple_of(j * size, size), size)


def ag_qkv_kernel(n_tp, n_cp, n_heads, x_ref, g_ref, wq_hbm, wk_hbm, wv_hbm, cos_ref, sin_ref, q_hbm, kv_hbm,
                  gath, wraw, wcat, q_ref, kv_own, ag_send, ag_recv, kv_send, kv_recv, out_sem, local):
    ag = Gather(n_tp, lambda half: gath.at[0, pl.ds(half * 128, 128)], gath, ag_send, ag_recv)
    cp = lax.axis_index('cp')
    up, down = (cp + 1) % n_cp, (cp + n_cp - 1) % n_cp
    hd = 128
    qw = n_heads * hd
    n_pieces = kv_own.shape[0]
    n_steps = n_pieces // 2
    width = gath.shape[2]

    loads = [
        pltpu.make_async_copy(wq_hbm, wraw, local.at[0]),
        pltpu.make_async_copy(wk_hbm, wcat.at[:, pl.ds(qw, hd)], local.at[1]),
        pltpu.make_async_copy(wv_hbm, wcat.at[:, pl.ds(qw + hd, hd)], local.at[2]),
    ]
    for c in loads:
        c.start()

    def norm(half):
        @pl.loop(0, 8)
        def _(r):
            x = x_ref[chunk(half * 8 + r, 16), :].astype(jnp.float32)
            mean_sq = jnp.sum(x * x, axis=-1, keepdims=True) / width
            gath[0, chunk(half * 8 + r, 16), :] = (x * lax.rsqrt(mean_sq + NORM_EPS) * g_ref[0:1, :]).astype(jnp.bfloat16)

    with jax.named_scope('norm'):
        norm(0)
    with jax.named_scope('greet'):
      greet(pltpu.get_barrier_semaphore(), [{'tp': ag.other}, {'tp': ag.right}, {'tp': ag.left}, {'cp': up}, {'cp': down}])
    ag.start(0)
    norm(1)
    ag.start(1)

    def place(n):
        return ag.place(2 * pair_of(n // 4) + n % 2, (n // 2) % 2)

    def kv_piece(where, n):
        slot, half = place(n)
        return kv_hbm.at[where, slot, half]

    def kv_copy(src, where, n, kind, lane, dst):
        return remote(src, kv_piece(where, n), kv_send.at[lane, n], kv_recv.at[kind, n], cp=dst)

    def kv_forward(n):
        kv_copy(kv_own.at[n], down, n, 0, 0, up).wait_recv()
        kv_copy(kv_own.at[n], up, n, 1, 0, up).wait_recv()
        odd = n % 2
        source = down * (1 - odd) + up * odd
        kv_copy(kv_piece(source, n), source, n, 2, 2, up * (1 - odd) + down * odd).start()

    def outs(n):
        slot, half = place(n)
        return (pltpu.make_async_copy(kv_own.at[n], kv_piece(cp, n), out_sem.at[0, n]),
                pltpu.make_async_copy(q_ref.at[n], q_hbm.at[slot, half], out_sem.at[1, n]))

    with jax.named_scope('wload'):
      for c in loads:
        c.wait()

    with jax.named_scope('wcat'):
        @pl.loop(0, wraw.shape[0] // 128)
        def _(i):
            block = wraw[chunk(i, 128)]
            for h in range(n_heads):
                wcat[chunk(i, 128), h * hd:(h + 1) * hd] = block[:, h, :]

    fine = pl.ds(cos_ref.shape[0] - 128, 128)

    @pl.loop(0, n_steps)
    def _(s):
        for k in range(n_steps):
            @pl.when(s == k)
            def _():
                with jax.named_scope(f'take{k}'):
                    ag.take(k // 2, k % 2)
        acc = jnp.dot(gath[s // 2, chunk(s % 2, 256), :], wcat[...], preferred_element_type=jnp.float32)
        for i in range(2):
            n = 2 * s + i
            slot, half = place(n)
            part = acc[i * 128:(i + 1) * 128, :]
            coarse = pl.ds(slot * 2 + half, 1)
            cos0, sin0 = cos_ref[coarse, :], sin_ref[coarse, :]
            cos = cos0 * cos_ref[fine, :] - sin0 * sin_ref[fine, :]
            sin = sin0 * cos_ref[fine, :] + cos0 * sin_ref[fine, :]

            def rope(t):
                t = t.astype(jnp.bfloat16).astype(jnp.float32)
                return (t * cos + pltpu.roll(t, hd // 2, 1) * sin).astype(jnp.bfloat16)

            kv_own[n, 0] = rope(part[:, qw:qw + hd])
            kv_own[n, 1] = part[:, qw + hd:].T.astype(jnp.bfloat16)
            for h in range(n_heads):
                q_ref[n, h] = rope(part[:, h * hd:(h + 1) * hd]).astype(jnp.float32).T.astype(jnp.bfloat16)
        for i in range(2):
            n = 2 * s + i
            kv_copy(kv_own.at[n], cp, n, 0, 0, up).start()
            kv_copy(kv_own.at[n], cp, n, 1, 1, down).start()
            for c in outs(n):
                c.start()

        @pl.when(s >= 2)
        def _():
            kv_forward(2 * s - 4)
            kv_forward(2 * s - 3)

    with jax.named_scope('kvtail'):
        @pl.loop(n_pieces - 4, n_pieces)
        def _(n):
            kv_forward(n)

        @pl.loop(0, n_pieces)
        def _(n):
            kv_copy(kv_own.at[n], (cp + 2) % n_cp, n, 2, 0, up).wait_recv()
            for c in outs(n):
                c.wait()
            for lane in range(3):
                kv_copy(kv_own.at[n], cp, n, 0, lane, up).wait_send()
    ag.finish()


def ag_qkv(x_rows, gains, w_q, w_k, w_v, n_tp, n_cp):
    rows, width = x_rows.shape
    n_heads, hd = w_q.shape[1:]
    bf = jnp.bfloat16
    piece = rows * n_tp // 2
    n = jnp.arange(2 * n_tp, dtype=jnp.int32)
    late = n // n_tp
    cp = lax.axis_index('cp')
    firsts = (cp * (1 - late) + (2 * n_cp - 1 - cp) * late) * piece + (n % n_tp) * 128
    points = jnp.concatenate([firsts, jnp.arange(128, dtype=jnp.int32)]).astype(jnp.float32)
    lane = jnp.arange(hd, dtype=jnp.int32)
    freq = ROPE_THETA ** (-2.0 * (lane % (hd // 2)).astype(jnp.float32) / hd)
    angles = points[:, None] * freq[None, :]
    sign = jnp.where(lane < hd // 2, -1.0, 1.0)
    return pl.pallas_call(
        functools.partial(ag_qkv_kernel, n_tp, n_cp, n_heads),
        out_shape=(jax.ShapeDtypeStruct((n_tp, 2, n_heads, hd, 128), bf),
                   jax.ShapeDtypeStruct((n_cp, n_tp, 2, 2, 128, hd), bf)),
        in_specs=[VM, VM, HBM, HBM, HBM, VM, VM],
        out_specs=(HBM, HBM),
        scratch_shapes=[
            pltpu.VMEM((4, 2 * rows, width), bf),
            pltpu.VMEM(w_q.shape, bf),
            pltpu.VMEM((width, (n_heads + 2) * hd), bf),
            pltpu.VMEM((16, n_heads, hd, 128), bf),
            pltpu.VMEM((16, 2, 128, hd), bf),
            *Gather.sems(),
            pltpu.SemaphoreType.DMA((3, 16)),
            pltpu.SemaphoreType.DMA((3, 16)),
            pltpu.SemaphoreType.DMA((2, 16)),
            pltpu.SemaphoreType.DMA((3,)),
        ],
        compiler_params=params(0),
        name='ag_qkv',
    )(x_rows, gains, w_q, w_k, w_v, jnp.cos(angles), jnp.sin(angles) * sign)


KEY_BLOCK = 512
EXP_ROWS = 64


def attend(q_tile, kv_ref, n_full, shift, n_cp, n_tp, sa_ref, sb_ref, p_ref, acc_ref, m_ref, l_ref):
    hd, nq = q_tile.shape
    c = LOG2E * hd ** -0.5
    per_piece = n_tp * 256 // 2 // KEY_BLOCK

    def place(n):
        piece = n // per_piece
        late = piece // n_cp
        return piece * (1 - late) + (2 * n_cp - 1 - piece) * late, (n % per_piece) * (KEY_BLOCK // 256) + late * (n_tp // 2)

    def scores(n, dst, masked=False):
        j, t = place(n)
        keys = kv_ref[j, pl.ds(t, KEY_BLOCK // 256), :, 0].reshape(KEY_BLOCK, hd)
        s = jnp.dot(keys, q_tile, preferred_element_type=jnp.float32)
        if masked:
            key = lax.broadcasted_iota(jnp.int32, s.shape, 0)
            row = lax.broadcasted_iota(jnp.int32, s.shape, 1) % 128
            s = jnp.where(key <= row + shift, s, -1e30)
        dst[...] = s

    def process(n, s_ref):
        j, t = place(n)
        m8 = jnp.max(s_ref[...].reshape(KEY_BLOCK // 8, 8, nq), axis=0)
        m = m_ref[...]
        m_new = jnp.maximum(m, jnp.max(m8, axis=0, keepdims=True))
        m_ref[...] = m_new
        alpha = jnp.exp2((m - m_new) * c)
        mc = m_new * c
        l8 = l_ref[...] * alpha
        for r in range(0, KEY_BLOCK, EXP_ROWS):
            p = jnp.exp2(s_ref[r:r + EXP_ROWS, :] * c - mc)
            l8 = l8 + jnp.sum(p.reshape(EXP_ROWS // 8, 8, nq), axis=0)
            p_ref[r:r + EXP_ROWS, :] = p.astype(jnp.bfloat16)
        l_ref[...] = l8
        v_t = jnp.concatenate([kv_ref[j, t + i // 2, i % 2, 1] for i in range(KEY_BLOCK // 128)], axis=1)
        acc_ref[...] = acc_ref[...] * alpha + jnp.dot(v_t, p_ref[...], preferred_element_type=jnp.float32)

    acc_ref[...] = jnp.zeros_like(acc_ref)
    m_ref[...] = jnp.full(m_ref.shape, -1e30, jnp.float32)
    l_ref[...] = jnp.zeros_like(l_ref)
    scores(n_full, sa_ref, True)

    @pl.loop(0, n_full // 2)
    def _(k):
        later = (k + 1023) // 1024
        scores(2 * k, sb_ref)
        process(n_full * (1 - later) + (2 * k - 1) * later, sa_ref)
        scores(2 * k + 1, sa_ref)
        process(2 * k, sb_ref)

    later = (n_full // 2 + 1023) // 1024
    held = n_full * (1 - later) + (2 * (n_full // 2) - 1) * later

    @pl.when(n_full % 2 == 1)
    def _():
        scores(n_full - 1, sb_ref)
        process(held, sa_ref)
        process(n_full - 1, sb_ref)

    @pl.when(n_full % 2 == 0)
    def _():
        process(held, sa_ref)

    return acc_ref[...] / jnp.sum(l_ref[...], axis=0, keepdims=True)


CHUNK = 1024
UNITS = 8


class Reduce(Chips):
    def __init__(self, n_tp, txp, rxp, land, peer_sem, ring_sem):
        super().__init__(n_tp)
        self.txp, self.rxp, self.land, self.peer_sem, self.ring_sem = txp, rxp, land, peer_sem, ring_sem
        self.n_chunks = rxp.shape[1]

    def to_other(self, o, j):
        return remote(self.txp.at[o % 2, j], self.rxp.at[o, j], self.peer_sem.at[0, o, j], self.peer_sem.at[1, o, j], tp=self.other)

    def onward(self, o, j):
        odd = o % 2
        return remote(self.rxp.at[o, j], self.land.at[o, j], self.ring_sem.at[0, o, j], self.ring_sem.at[1, o, j],
                      tp=self.right * (1 - odd) + self.left * odd)

    def give(self, o, j, value):
        self.txp[o % 2, j] = value.astype(jnp.bfloat16)
        self.to_other(o, j).start()

    def given(self, o):
        @pl.loop(0, self.n_chunks)
        def _(j):
            self.to_other(o, j).wait_send()

    def keep(self, o, j, value):
        self.to_other(o, j).wait_recv()
        self.rxp[o, j] = (value + self.rxp[o, j].astype(jnp.float32)).astype(jnp.bfloat16)

    def late(self, o, j):
        self.onward(o - 4, j).wait_recv()
        self.rxp[o, j] = (self.rxp[o, j].astype(jnp.float32) + self.land[o - 4, j].astype(jnp.float32)).astype(jnp.bfloat16)

    def total(self, half, j, rows):
        a, b = (4, 3) if half == 0 else (2, 5)
        return (self.rxp[6 + half, j, rows, :].astype(jnp.float32) + self.land[a, j, rows, :].astype(jnp.float32)
                + self.land[b, j, rows, :].astype(jnp.float32)).astype(jnp.bfloat16).astype(jnp.float32)

    def arrive(self, j):
        for o in range(2, 6):
            self.onward(o, j).wait_recv()

    def finish(self):
        @pl.loop(0, self.n_chunks)
        def _(j):
            for o in range(6):
                self.onward(o, j).wait_send()


def rs_scratch(width):
    bf = jnp.bfloat16
    n = width // CHUNK
    return [
        pltpu.VMEM((2, n, 128, CHUNK), bf),
        pltpu.VMEM((UNITS, n, 128, CHUNK), bf),
        pltpu.VMEM((6, n, 128, CHUNK), bf),
        pltpu.SemaphoreType.DMA((2, UNITS, n)),
        pltpu.SemaphoreType.DMA((2, 6, n)),
    ]


def greet_tp(r):
    greet(pltpu.get_barrier_semaphore(), [{'tp': r.other}, {'tp': r.right}, {'tp': r.left}])


def attn_out_kernel(n_tp, n_cp, q_hbm, kv_hbm, wo_hbm, x_ref, g_ref, y_ref, b_ref,
                    q_ref, kv_ref, wo, a_tile, q_tile, sa, sb, p, acc, m, l, sq, w_sem, q_sem, *rs):
    cp = lax.axis_index('cp')
    width = x_ref.shape[1]
    hd = q_tile.shape[0]
    n_heads = q_ref.shape[2]
    piece = n_tp * 128
    n_chunks = width // CHUNK
    red = Reduce(n_tp, *rs)
    loads = [pltpu.make_async_copy(kv_hbm, kv_ref, q_sem.at[0]), pltpu.make_async_copy(q_hbm, q_ref, q_sem.at[1]),
             pltpu.make_async_copy(wo_hbm, wo, w_sem)]
    for c in loads:
        c.start()
    greet_tp(red)
    for c in loads:
        c.wait()

    def order(i):
        first = 1 - i // 4
        turn = 2 * (1 - red.chip // (red.n_chips // 2))
        return first * ((i + turn) % 4) + (1 - first) * i

    @pl.loop(0, 2 * UNITS)
    def _(u):
        o = order(u // 2)
        flip = 1 - u % 2
        slot, half = red.place(o, flip)
        late = slot // (n_tp // 2)
        first = (cp * (1 - late) + (2 * n_cp - 1 - cp) * late) * piece + (slot % (n_tp // 2)) * 256 + half * 128
        for h in range(n_heads):
            q_tile[:, h * 128:(h + 1) * 128] = q_ref[slot, half, h]
        with jax.named_scope('attend'):
            out = attend(q_tile[...], kv_ref, first // KEY_BLOCK, first % KEY_BLOCK, n_cp, n_tp, sa, sb, p, acc, m, l)
        for h in range(n_heads):
            a_tile[:, h * hd:(h + 1) * hd] = out[:, h * 128:(h + 1) * 128].T.astype(jnp.bfloat16)

        def product(j):
            return jnp.dot(a_tile[...], wo[:, chunk(j, CHUNK)], preferred_element_type=jnp.float32)

        @pl.when(flip == 1)
        def _():
            @pl.when(u >= 4)
            def _():
                red.given(order(u // 2 - 2))

            with jax.named_scope('give'):
                @pl.loop(0, n_chunks)
                def _(j):
                    red.give(o, j, product(j))

        @pl.when(flip == 0)
        def _():
            with jax.named_scope('keep'):
                @pl.loop(0, n_chunks)
                def _(j):
                    red.keep(o, j, product(j))

                    @pl.when(o // 2 == 2)
                    def _():
                        red.late(o, j)

                    @pl.when(o < 6)
                    def _():
                        red.onward(o, j).start()

    sq[...] = jnp.zeros_like(sq)

    @pl.loop(0, n_chunks)
    def _(j):
        with jax.named_scope('arrive'):
            red.arrive(j)
        for half in range(2):
            @pl.loop(0, 8)
            def _(r):
                rows = chunk(r, 16)
                at = chunk(half * 8 + r, 16)
                y = (x_ref[at, chunk(j, CHUNK)].astype(jnp.float32) + red.total(half, j, rows)).astype(jnp.bfloat16)
                y_ref[at, chunk(j, CHUNK)] = y
                yf = y.astype(jnp.float32)
                y2 = yf * yf
                sq[at, :] += sum(y2[:, i * 128:(i + 1) * 128] for i in range(CHUNK // 128))

    @pl.loop(0, 16)
    def _(r):
        at = chunk(r, 16)
        scale = lax.rsqrt(jnp.sum(sq[at, :], axis=-1, keepdims=True) / width + NORM_EPS)
        b_ref[at, :] = (y_ref[at, :].astype(jnp.float32) * scale * g_ref[1:2, :]).astype(jnp.bfloat16)
    red.given(6)
    red.given(7)
    red.finish()


def attn_out(q, kv, w_o, x_rows, gains, n_tp, n_cp):
    bf = jnp.bfloat16
    rows, width = x_rows.shape
    n_heads, hd = q.shape[2], q.shape[3]
    nq = n_heads * 128
    return pl.pallas_call(
        functools.partial(attn_out_kernel, n_tp, n_cp),
        out_shape=(jax.ShapeDtypeStruct((rows, width), bf),) * 2,
        in_specs=[HBM, HBM, HBM, VM, VM],
        out_specs=(VM, VM),
        scratch_shapes=[
            pltpu.VMEM(q.shape, bf),
            pltpu.VMEM(kv.shape, bf),
            pltpu.VMEM((n_heads * hd, width), bf),
            pltpu.VMEM((128, n_heads * hd), bf),
            pltpu.VMEM((hd, nq), bf),
            pltpu.VMEM((KEY_BLOCK, nq), jnp.float32),
            pltpu.VMEM((KEY_BLOCK, nq), jnp.float32),
            pltpu.VMEM((KEY_BLOCK, nq), bf),
            pltpu.VMEM((hd, nq), jnp.float32),
            pltpu.VMEM((1, nq), jnp.float32),
            pltpu.VMEM((8, nq), jnp.float32),
            pltpu.VMEM((rows, 128), jnp.float32),
            pltpu.SemaphoreType.DMA(()),
            pltpu.SemaphoreType.DMA((2,)),
            *rs_scratch(width),
        ],
        compiler_params=params(1),
        name='attn_out',
    )(q, kv, w_o, x_rows, gains)


TILE = 256
COLS = 512
N_W = 2
N_D = 3


def mlp_kernel(n_tp, b_hbm, wg_hbm, wu_hbm, wd_hbm, y_hbm, z_hbm, gath, hid, w, wd, ag_send, ag_recv, w_sem, wd_sem, io_sem, z_sem, *rs):
    red = Reduce(n_tp, *rs)
    ag = Gather(n_tp, lambda half: b_hbm.at[pl.ds(half * 128, 128)], gath, ag_send, ag_recv)
    rows, width = b_hbm.shape
    n_tiles = hid.shape[2] // TILE
    n_cols = width // COLS
    per_chunk = CHUNK // COLS
    own_loads = [pltpu.make_async_copy(ag.src(half), ag.part(0, half), io_sem.at[half]) for half in range(2)]
    for c in own_loads:
        c.start()

    def w_load(g, part):
        src = (wg_hbm, wu_hbm)[part]
        return pltpu.make_async_copy(src.at[:, chunk(g % n_tiles, TILE)], w.at[g % N_W, :, pl.ds(part * TILE, TILE)], w_sem.at[g % N_W, part])

    def w_start(g):
        w_load(g, 0).start()
        w_load(g, 1).start()

    def wd_load(c):
        return pltpu.make_async_copy(wd_hbm.at[:, chunk(c % n_cols, COLS)], wd.at[c % N_D], wd_sem.at[c % N_D])

    with jax.named_scope('mgreet'):
        greet_tp(red)
    ag.start(0)
    ag.start(1)
    for g in range(N_W):
        w_start(g)
    for c in range(N_D):
        wd_load(c).start()

    def gate_up(b):
        where = b - 2 * (b // 3)
        base = b * n_tiles

        @pl.loop(0, n_tiles)
        def _(i):
            w_load(base + i, 0).wait()
            w_load(base + i, 1).wait()
            both = jnp.dot(gath[b], w[(base + i) % N_W], preferred_element_type=jnp.float32)
            gate, up = both[:, :TILE], both[:, TILE:]
            hid[where, :, chunk(i, TILE)] = (gate / (1.0 + jnp.exp(-gate)) * up).astype(jnp.bfloat16)
            w_start(base + i + N_W)

    def down(t, pair, flip):
        with jax.named_scope(f'down{t}'):
            down_pass(t, pair, flip)

    def down_pass(t, pair, flip):
        where = (1, 1, 2, 0)[pair]

        @pl.loop(0, n_cols)
        def _(c):
            n = t * n_cols + c
            wd_load(n).wait()
            part = jnp.dot(hid[where, pl.ds(flip * rows, rows), :], wd[n % N_D], preferred_element_type=jnp.float32)
            wd_load(n + N_D).start()
            j, at = c // per_chunk, chunk(c % per_chunk, COLS)
            last = c % per_chunk == per_chunk - 1
            for i in range(2):
                o = 2 * pair + i
                mine = part[i * 128:(i + 1) * 128, :]
                if flip:
                    red.txp[i, j, :, at] = mine.astype(jnp.bfloat16)

                    @pl.when(last)
                    def _():
                        red.to_other(o, j).start()
                else:
                    @pl.when(c % per_chunk == 0)
                    def _():
                        red.to_other(o, j).wait_recv()
                    red.rxp[o, j, :, at] = (mine + red.rxp[o, j, :, at].astype(jnp.float32)).astype(jnp.bfloat16)
                    if pair < 2:
                        @pl.when(last)
                        def _():
                            red.onward(o, j).start()

    def given(pair):
        red.given(2 * pair)
        red.given(2 * pair + 1)

    with jax.named_scope('own'):
        for c in own_loads:
            c.wait()

    @pl.loop(0, 4)
    def _(b):
        for k in range(4):
            @pl.when(b == k)
            def _():
                with jax.named_scope(f'take{k}'):
                    if k == 3:
                        ag.take(k, 0)
                    ag.take(k, 1)
        with jax.named_scope('gate_up'):
            gate_up(b)

        @pl.when(b == 0)
        def _():
            ag.take(1, 0)
            down(0, 3, 1)
            given(3)

        @pl.when(b == 1)
        def _():
            down(1, 1, 1)
            ag.take(2, 0)
            down(2, 1, 0)
            given(1)

    ag.finish()
    y_loads = [pltpu.make_async_copy(y_hbm.at[pl.ds(half * 128, 128)], ag.part(0, half), io_sem.at[half]) for half in range(2)]
    for c in y_loads:
        c.start()
    down(3, 0, 1)
    down(4, 0, 0)
    given(0)
    down(5, 2, 1)
    down(6, 2, 0)
    given(2)
    down(7, 3, 0)
    for i in range(N_D):
        wd_load(UNITS * n_cols + i).wait()
    for i in range(N_W):
        for part in range(2):
            w_load(4 * n_tiles + i, part).wait()

    @pl.loop(0, red.n_chunks)
    def _(j):
        for o in (4, 5):
            red.late(o, j)
            red.onward(o, j).start()
    for c in y_loads:
        c.wait()

    def z_out(j, half):
        return pltpu.make_async_copy(gath.at[0, pl.ds((2 + half) * 128, 128), chunk(j, CHUNK)], z_hbm.at[pl.ds(half * 128, 128), chunk(j, CHUNK)], z_sem.at[half, j])

    @pl.loop(0, red.n_chunks)
    def _(j):
        red.arrive(j)
        for half in range(2):
            @pl.loop(0, 8)
            def _(r):
                at = chunk(r, 16)
                y = gath[0, chunk(half * 8 + r, 16), chunk(j, CHUNK)].astype(jnp.float32)
                gath[0, chunk(16 + half * 8 + r, 16), chunk(j, CHUNK)] = (y + red.total(half, j, at)).astype(jnp.bfloat16)
            z_out(j, half).start()

    @pl.loop(0, red.n_chunks)
    def _(j):
        for half in range(2):
            z_out(j, half).wait()
    red.finish()


def mlp(b, w_gate, w_up, w_down, y_rows, n_tp):
    bf = jnp.bfloat16
    rows, width = b.shape
    ffn = w_gate.shape[1]
    return pl.pallas_call(
        functools.partial(mlp_kernel, n_tp),
        out_shape=jax.ShapeDtypeStruct((rows, width), bf),
        in_specs=[HBM] * 5,
        out_specs=HBM,
        scratch_shapes=[
            pltpu.VMEM((4, 2 * rows, width), bf),
            pltpu.VMEM((3, 2 * rows, ffn), bf),
            pltpu.VMEM((N_W, width, 2 * TILE), bf),
            pltpu.VMEM((N_D, ffn, COLS), bf),
            *Gather.sems(),
            pltpu.SemaphoreType.DMA((N_W, 2)),
            pltpu.SemaphoreType.DMA((N_D,)),
            pltpu.SemaphoreType.DMA((2,)),
            pltpu.SemaphoreType.DMA((2, width // CHUNK)),
            *rs_scratch(width),
        ],
        compiler_params=params(2),
        name='mlp',
    )(b, w_gate, w_up, w_down, y_rows)


def solution(mesh):
    n_cp, n_tp = mesh.shape['cp'], mesh.shape['tp']
    row_spec = P('dp', ('cp', 'tp'), None)
    head_cols = P(None, 'tp', None)

    def local_layer(x, g_attn, w_q, w_k, w_v, w_o, g_mlp, w_gate, w_up, w_down):
        x_rows = x[0]
        gains = jnp.stack([g_attn, g_mlp]).astype(jnp.float32)
        q, kv = ag_qkv(x_rows, gains, w_q, w_k[:, 0], w_v[:, 0], n_tp, n_cp)
        y, b = attn_out(q, kv, w_o.reshape(-1, x_rows.shape[1]), x_rows, gains, n_tp, n_cp)
        return mlp(b, w_gate, w_up, w_down, y, n_tp)[None]

    return jax.shard_map(local_layer, mesh=mesh,
                         in_specs=(row_spec, P(), head_cols, head_cols, head_cols, P('tp', None, None),
                                   P(), P(None, 'tp'), P(None, 'tp'), P('tp', None)),
                         out_specs=row_spec, check_vma=False)
```

```python
import functools

import jax
import jax.numpy as jnp
from jax import lax
from jax.experimental import pallas as pl
from jax.experimental.pallas import tpu as pltpu
from jax.sharding import PartitionSpec as P

NORM_EPS = 1e-5
ROPE_THETA = 500000.0
MESH = pl.DeviceIdType.MESH
VMEM_LIMIT = 67_000_000
LOG2E = 1.4426950408889634
BLOCK = 128
SUB = 16
HIGH = 1024
VM = pl.BlockSpec(memory_space=pltpu.VMEM)
HBM = pl.BlockSpec(memory_space=pl.ANY)


def params(ident):
    return pltpu.CompilerParams(collective_id=ident, has_side_effects=True, vmem_limit_bytes=VMEM_LIMIT)


def remote(src, dst, send_sem, recv_sem, **where):
    return pltpu.make_async_remote_copy(
        src_ref=src, dst_ref=dst, send_sem=send_sem, recv_sem=recv_sem,
        device_id=where, device_id_type=MESH)


def ring(n_tp):
    n_chips = n_tp // 2
    me = lax.axis_index('tp')
    chip, core = me // 2, me % 2
    other = chip * 2 + (1 - core)
    right = ((chip + 1) % n_chips) * 2 + core
    left = ((chip + n_chips - 1) % n_chips) * 2 + core
    return me, chip, core, other, right, left


def greet(barrier, partners, meanwhile=lambda: None):
    for where in partners:
        pl.semaphore_signal(barrier, inc=1, device_id=where, device_id_type=MESH)
    meanwhile()
    pl.semaphore_wait(barrier, len(partners))


def unit_place(o):
    far = (7 - o) // 6
    near = o // 6
    offset = 2 * far + (1 - far - near) * (1 - 2 * (o % 2))
    half = (o % 2 + ((o // 2) % 2) * (1 - o // 4)) % 2
    return offset, half


def pair_of(b):
    mid = ((b + 1) // 2) % 2
    return mid * b + (1 - mid) * (3 - b)


class Chips:
    def __init__(self, n_tp):
        self.n_chips = n_tp // 2
        self.me, self.chip, self.core, self.other, self.right, self.left = ring(n_tp)

    def place(self, o, flip):
        offset, half = unit_place(o)
        return ((self.chip + offset + self.n_chips) % self.n_chips) * 2 + (self.core + flip) % 2, half


class Gather(Chips):
    def __init__(self, n_tp, src, gath, send_sem, recv_sem):
        super().__init__(n_tp)
        self.src, self.gath, self.send_sem, self.recv_sem = src, gath, send_sem, recv_sem

    @staticmethod
    def sems():
        return [pltpu.SemaphoreType.DMA((2, 4, 4)), pltpu.SemaphoreType.DMA((4, 4))]

    def part(self, b, e):
        return self.gath.at[b, pl.ds(e * BLOCK, BLOCK)]

    def copy(self, src, b, e, dst, lane=1):
        return remote(src, self.part(b, e), self.send_sem.at[lane, b, e], self.recv_sem.at[b, e], tp=dst)

    def start(self, half):
        self.copy(self.src(half), 1, 1 - half, (self.right, self.left)[half]).start()
        self.copy(self.src(half), 0, 2 + half, self.other, 0).start()
        if half:
            self.copy(self.src(1), 2, 1, self.right).start()
            self.copy(self.src(0), 2, 0, self.left).start()

    def take(self, b, flip):
        for i in range(2):
            e = 2 * flip + i
            here = self.part(b, e)
            if flip or b:
                self.copy(here, b, e, self.other).wait_recv()
            if b and not flip:
                if b == 1:
                    self.copy(here, 3, 1 - i, (self.left, self.right)[i]).start()
                self.copy(here, b, 2 + i, self.other, 0).start()

    def finish(self):
        for i in range(2):
            for b in range(4):
                self.copy(self.src(0), b, 2 + i, self.other, 0).wait_send()
                if b:
                    self.copy(self.src(0), b, i, self.other).wait_send()


def chunk(j, size):
    return pl.ds(j * size if isinstance(j, int) else pl.multiple_of(j * size, size), size)


KEY_BLOCK = 512
HIDDEN = -1e30
EXP_ROWS = 64


class Attend:
    def __init__(self, q_tile, kv_ref, n_cp, n_tp, buffers, p_ref, acc_ref, m_ref, l_ref):
        self.q_tile, self.kv_ref, self.n_cp, self.n_tp = q_tile, kv_ref, n_cp, n_tp
        self.buffers, self.p_ref, self.acc_ref, self.m_ref, self.l_ref = buffers, p_ref, acc_ref, m_ref, l_ref
        self.c = LOG2E * q_tile.shape[0] ** -0.5

    def reset(self):
        self.acc_ref[...] = jnp.zeros_like(self.acc_ref)
        self.m_ref[...] = jnp.full(self.m_ref.shape, HIDDEN, jnp.float32)
        self.l_ref[...] = jnp.zeros_like(self.l_ref)

    def place(self, n):
        per_piece = self.n_tp * BLOCK // KEY_BLOCK
        piece = n // per_piece
        late = piece // self.n_cp
        block = piece * (1 - late) + (2 * self.n_cp - 1 - piece) * late
        return block, (n % per_piece) * (KEY_BLOCK // 256) + late * (self.n_tp // 2)

    def scores(self, n, dst, shift=None):
        j, t = self.place(n)
        q = self.q_tile[...]
        keys = self.kv_ref[j, pl.ds(t, KEY_BLOCK // 256), :, 0].reshape(KEY_BLOCK, q.shape[0])
        s = jnp.dot(keys, q, preferred_element_type=jnp.float32)
        if shift is not None:
            row = lax.broadcasted_iota(jnp.int32, s.shape, 1) % BLOCK
            s = jnp.where(lax.broadcasted_iota(jnp.int32, s.shape, 0) <= row + shift, s, HIDDEN)
        dst[...] = s

    def process(self, n, s_ref):
        j, t = self.place(n)
        nq = s_ref.shape[1]
        m8 = jnp.max(s_ref[...].reshape(-1, 8, nq), axis=0)
        m = self.m_ref[...]
        m_new = jnp.maximum(m, jnp.max(m8, axis=0, keepdims=True))
        self.m_ref[...] = m_new
        alpha = jnp.exp2((m - m_new) * self.c)
        mc = m_new * self.c
        l8 = self.l_ref[...] * alpha
        for r in range(0, KEY_BLOCK, EXP_ROWS):
            p = jnp.exp2(s_ref[r:r + EXP_ROWS, :] * self.c - mc)
            l8 = l8 + jnp.sum(p.reshape(-1, 8, nq), axis=0)
            self.p_ref[r:r + EXP_ROWS, :] = p.astype(jnp.bfloat16)
        self.l_ref[...] = l8
        v_t = jnp.concatenate([self.kv_ref[j, t + i // 2, i % 2, 1] for i in range(KEY_BLOCK // BLOCK)], axis=1)
        self.acc_ref[...] = self.acc_ref[...] * alpha + jnp.dot(v_t, self.p_ref[...], preferred_element_type=jnp.float32)

    def sweep(self, start, shift, count, base, step):
        sa, sb = self.buffers

        self.scores(start, sa, shift)

        @pl.loop(0, count // 2)
        def _(k):
            fresh = 1 - (k + HIGH - 1) // HIGH
            self.scores(base + step * 2 * k, sb)
            self.process(fresh * start + (1 - fresh) * (base + step * (2 * k - 1)), sa)
            self.scores(base + step * (2 * k + 1), sa)
            self.process(base + step * 2 * k, sb)

        even = count // 2 * 2
        fresh = 1 - (even + HIGH - 1) // HIGH
        held = fresh * start + (1 - fresh) * (base + step * (even - 1))

        @pl.when(count % 2 == 1)
        def _():
            self.scores(base + step * even, sb)
            self.process(held, sa)
            self.process(base + step * even, sb)

        @pl.when(count % 2 == 0)
        def _():
            self.process(held, sa)

    def sweep_if_any(self, count, base, step):
        @pl.when(count > 0)
        def _():
            self.sweep(base, None, count - 1, base + step, step)

    def result(self):
        return self.acc_ref[...] / jnp.sum(self.l_ref[...], axis=0, keepdims=True)


CHUNK = 1024
UNITS = 8


class Reduce(Chips):
    def __init__(self, n_tp, n_chunks, txp, rxp, land, peer_sem, ring_sem):
        super().__init__(n_tp)
        self.n_chunks = n_chunks
        self.txp = lambda o, j: txp.at[o % 2, :, chunk(j, CHUNK)]
        self.rxp = lambda o, j: rxp(o).at[:, chunk(j, CHUNK)]
        self.land = lambda o, j: land(o).at[:, chunk(j, CHUNK)]
        self.peer_sem, self.ring_sem = peer_sem, ring_sem

    def to_other(self, o, j):
        return remote(self.txp(o, j), self.rxp(o, j), self.peer_sem.at[0, o, j], self.peer_sem.at[1, o, j], tp=self.other)

    def onward(self, o, j):
        odd = o % 2
        return remote(self.rxp(o, j), self.land(o, j), self.ring_sem.at[0, o, j], self.ring_sem.at[1, o, j],
                      tp=self.right * (1 - odd) + self.left * odd)

    def give(self, o, j, value):
        self.txp(o, j)[...] = value.astype(jnp.bfloat16)
        self.to_other(o, j).start()

    def given(self, o):
        @pl.loop(0, self.n_chunks)
        def _(j):
            self.to_other(o, j).wait_send()

    def keep(self, o, j, value):
        self.to_other(o, j).wait_recv()
        self.rxp(o, j)[...] = (value + self.rxp(o, j)[...].astype(jnp.float32)).astype(jnp.bfloat16)

    def late(self, o, j):
        self.onward(o - 4, j).wait_recv()
        self.rxp(o, j)[...] = (self.rxp(o, j)[...].astype(jnp.float32) + self.land(o - 4, j)[...].astype(jnp.float32)).astype(jnp.bfloat16)

    def total(self, half, j, rows):
        parts = self.rxp(6 + half, j), self.land((4, 2)[half], j), self.land((3, 5)[half], j)
        return sum(p[rows, :].astype(jnp.float32) for p in parts).astype(jnp.bfloat16).astype(jnp.float32)

    def arrive(self, j):
        for o in range(2, 6):
            self.onward(o, j).wait_recv()

    def finish(self):
        @pl.loop(0, self.n_chunks)
        def _(j):
            for o in range(6):
                self.onward(o, j).wait_send()


def rs_sems(n_chunks):
    return [pltpu.SemaphoreType.DMA((2, UNITS, n_chunks)), pltpu.SemaphoreType.DMA((2, 6, n_chunks))]


def greet_tp(r):
    greet(pltpu.get_barrier_semaphore(), [{'tp': r.other}, {'tp': r.right}, {'tp': r.left}])


def scaled(ref, scale, gain_ref, lane):
    return ref.astype(jnp.float32) * scale * gain_ref[lane:lane + 1, :].astype(jnp.float32)


def attn_kernel(n_tp, n_cp, n_heads, x_ref, ga_ref, gm_ref, wq_hbm, wk_hbm, wv_hbm, wo_hbm, cos_ref, sin_ref, y_hbm, b_hbm,
                gath, wraw, wcat, q_ref, kv_ref, wo, y_ref, b_ref, a_tile, q_tile, sa, sb, p, acc, m, l, sq, txp,
                ag_send, ag_recv, kv_send, kv_recv, local, out_sem, free, *rs):
    ag = Gather(n_tp, lambda half: gath.at[0, pl.ds(half * BLOCK, BLOCK)], gath, ag_send, ag_recv)
    width = gath.shape[2]
    n_chunks = width // CHUNK
    unit = lambda o: gath.at[o // 4, chunk(o % 4, BLOCK)]
    red = Reduce(n_tp, n_chunks, txp, unit, lambda o: unit(o + UNITS), *rs)
    cp = lax.axis_index('cp')
    up, down = (cp + 1) % n_cp, (cp + n_cp - 1) % n_cp
    hd = BLOCK
    qw = n_heads * hd
    n_pieces = q_ref.shape[0]
    n_steps = n_pieces // 2
    lanes = range(width // BLOCK)
    tp_partners = [{'tp': ag.other}, {'tp': ag.right}, {'tp': ag.left}]

    loads = [
        pltpu.make_async_copy(wq_hbm, wraw, local.at[0]),
        pltpu.make_async_copy(wk_hbm, wcat.at[:, pl.ds(qw, hd)], local.at[1]),
        pltpu.make_async_copy(wv_hbm, wcat.at[:, pl.ds(qw + hd, hd)], local.at[2]),
        pltpu.make_async_copy(wo_hbm, wo, local.at[3]),
    ]
    for c in loads:
        c.start()

    def norm(half):
        @pl.loop(0, 8)
        def _(r):
            x = x_ref[chunk(half * 8 + r, SUB), :].astype(jnp.float32)
            scale = lax.rsqrt(jnp.sum(x * x, axis=-1, keepdims=True) / width + NORM_EPS)
            for i in lanes:
                at = slice(i * BLOCK, (i + 1) * BLOCK)
                gath[0, chunk(half * 8 + r, SUB), at] = scaled(x[:, at], scale, ga_ref, i).astype(jnp.bfloat16)

    greet(pltpu.get_barrier_semaphore(), [*tp_partners, {'cp': up}, {'cp': down}], lambda: norm(0))
    ag.start(0)
    norm(1)
    ag.start(1)

    def place(n):
        return ag.place(2 * pair_of(n // 4) + n % 2, (n // 2) % 2)

    def kv_copy(where, n, kind, lane, dst):
        slot, half = place(n)
        piece = kv_ref.at[where, slot, half]
        return remote(piece, piece, kv_send.at[lane, n], kv_recv.at[kind, n], cp=dst)

    def kv_forward(n):
        kv_copy(down, n, 0, 0, up).wait_recv()
        kv_copy(up, n, 1, 0, up).wait_recv()
        odd = n % 2
        kv_copy(down * (1 - odd) + up * odd, n, 2, 2, up * (1 - odd) + down * odd).start()

    for c in loads:
        c.wait()

    with jax.named_scope('wcat'):
        @pl.loop(0, wraw.shape[0] // BLOCK)
        def _(i):
            block = wraw[chunk(i, BLOCK)]
            for h in range(n_heads):
                wcat[chunk(i, BLOCK), h * hd:(h + 1) * hd] = block[:, h, :]

    def kv_far(begin, end):
        @pl.loop(begin, end)
        def _(n):
            kv_copy((cp + 2) % n_cp, n, 2, 0, up).wait_recv()

    def order(i):
        o = (1 - i // 4) * ((i + 2) % 4) + i // 4 * i
        swap = 1 - (red.chip + 1) // 2 % 2
        return o + swap * (1 - 2 * (o % 2))

    def tile(o, flip):
        slot, half = red.place(o, flip)
        late = slot // (n_tp // 2)
        first = ((cp * (1 - late) + (2 * n_cp - 1 - cp) * late) * n_tp + slot % (n_tp // 2) * 2 + half) * BLOCK
        for h in range(n_heads):
            q_tile[:, h * BLOCK:(h + 1) * BLOCK] = q_ref[4 * pair_of(o // 2) + 2 * flip + o % 2, h]
        work = Attend(q_tile, kv_ref, n_cp, n_tp, (sa, sb), p, acc.at[flip], m.at[flip], l.at[flip])
        return work, first // KEY_BLOCK, first % KEY_BLOCK

    def far_blocks(n_full):
        half = red.n_chips // 2
        per_half = n_cp * half
        far_late = 1 - red.chip // half
        early = n_full - (n_full // per_half) * (n_full - per_half)
        late = n_full - early
        mixed = far_late * late + (1 - far_late) * early
        at, parity = far_late * per_half, red.chip % half
        return (((mixed - parity + 1) // 2, at + parity, 2),
                ((n_full - mixed, per_half - at, 1), ((mixed + parity) // 2, at + 1 - parity, 2)))

    fine = pl.ds(cos_ref.shape[0] - BLOCK, BLOCK)

    @pl.loop(0, n_steps)
    def _(s):
        for k in range(n_steps):
            @pl.when(s == k)
            def _():
                with jax.named_scope(f'take{k}'):
                    ag.take(k // 2, k % 2)
        product = jnp.dot(gath[s // 2, chunk(s % 2, 256), :], wcat[...], preferred_element_type=jnp.float32)
        for i in range(2):
            n = 2 * s + i
            slot, half = place(n)
            part = product[i * BLOCK:(i + 1) * BLOCK, :]
            coarse = pl.ds(slot * 2 + half, 1)
            cos0, sin0 = cos_ref[coarse, :], sin_ref[coarse, :]
            cos = cos0 * cos_ref[fine, :] - sin0 * sin_ref[fine, :]
            sin = sin0 * cos_ref[fine, :] + cos0 * sin_ref[fine, :]

            def rope(t):
                t = t.astype(jnp.bfloat16).astype(jnp.float32)
                return (t * cos + pltpu.roll(t, hd // 2, 1) * sin).astype(jnp.bfloat16)

            kv_ref[cp, slot, half, 0] = rope(part[:, qw:qw + hd])
            kv_ref[cp, slot, half, 1] = part[:, qw + hd:].T.astype(jnp.bfloat16)
            for h in range(n_heads):
                q_ref[n, h] = rope(part[:, h * hd:(h + 1) * hd]).astype(jnp.float32).T.astype(jnp.bfloat16)
        for i in range(2):
            kv_copy(cp, 2 * s + i, 0, 0, up).start()
            kv_copy(cp, 2 * s + i, 1, 1, down).start()

        @pl.when((s >= 1) & (s != n_steps - 2))
        def _():
            kv_forward(2 * s - 2)
            kv_forward(2 * s - 1)

        @pl.when(s == n_steps - 3)
        def _():
            with jax.named_scope('early'):
                kv_forward(2 * s)
                kv_forward(2 * s + 1)
                kv_far(0, n_pieces - 4)
                o = order(0)
                for flip in (1, 0):
                    work, n_full, _ = tile(o, flip)
                    far, others = far_blocks(n_full)
                    work.reset()
                    for blocks in others:
                        work.sweep_if_any(*blocks)

    ag.finish()
    for where in tp_partners:
        pl.semaphore_signal(free, inc=1, device_id=where, device_id_type=MESH)
    with jax.named_scope('kvtail'):
        for n in range(n_pieces - 2, n_pieces):
            kv_forward(n)

        kv_far(n_pieces - 4, n_pieces)
    pl.semaphore_wait(free, len(tp_partners))

    @pl.loop(0, 2 * UNITS)
    def _(u):
        o = order(u // 2)
        flip = 1 - u % 2
        work, n_full, shift = tile(o, flip)
        begun = 1 - (u + 2 * UNITS - 2) // (2 * UNITS)
        far, _ = far_blocks(n_full)

        @pl.when(begun == 0)
        def _():
            work.reset()
        with jax.named_scope('attend'):
            work.sweep(n_full, shift, *(begun * f + (1 - begun) * w for f, w in zip(far, (n_full, 0, 1))))
        out = work.result()
        for h in range(n_heads):
            a_tile[:, h * hd:(h + 1) * hd] = out[:, h * BLOCK:(h + 1) * BLOCK].T.astype(jnp.bfloat16)

        def product(j):
            return jnp.dot(a_tile[...], wo[:, chunk(j, CHUNK)], preferred_element_type=jnp.float32)

        @pl.when(flip == 1)
        def _():
            @pl.when(u >= 4)
            def _():
                red.given(order(u // 2 - 2))

            with jax.named_scope('give'):
                @pl.loop(0, n_chunks)
                def _(j):
                    red.give(o, j, product(j))

        @pl.when(flip == 0)
        def _():
            with jax.named_scope('keep'):
                @pl.loop(0, n_chunks)
                def _(j):
                    red.keep(o, j, product(j))

                    @pl.when(o < 4)
                    def _():
                        red.onward(o, j).start()

            @pl.when(u // 2 == 5 + red.chip // (red.n_chips // 2))
            def _():
                with jax.named_scope('late'):
                    @pl.loop(0, n_chunks)
                    def _(j):
                        for o in (4, 5):
                            red.late(o, j)
                            red.onward(o, j).start()

    sq[...] = jnp.zeros_like(sq)

    def y_out(j):
        return pltpu.make_async_copy(y_ref.at[:, chunk(j, CHUNK)], y_hbm.at[:, chunk(j, CHUNK)], out_sem.at[j])

    def b_out(i):
        return pltpu.make_async_copy(b_ref.at[chunk(i, 64)], b_hbm.at[chunk(i, 64)], out_sem.at[n_chunks + i])

    @pl.loop(0, n_chunks)
    def _(j):
        with jax.named_scope('arrive'):
            red.arrive(j)
        for half in range(2):
            @pl.loop(0, 8)
            def _(r):
                at = chunk(half * 8 + r, SUB)
                y = (x_ref[at, chunk(j, CHUNK)].astype(jnp.float32) + red.total(half, j, chunk(r, SUB))).astype(jnp.bfloat16)
                y_ref[at, chunk(j, CHUNK)] = y
                yf = y.astype(jnp.float32)
                y2 = yf * yf
                sq[at, :] += sum(y2[:, i * BLOCK:(i + 1) * BLOCK] for i in range(CHUNK // BLOCK))
        y_out(j).start()

    @pl.loop(0, SUB)
    def _(r):
        at = chunk(r, SUB)
        scale = lax.rsqrt(jnp.sum(sq[at, :], axis=-1, keepdims=True) / width + NORM_EPS)
        for i in lanes:
            to = slice(i * BLOCK, (i + 1) * BLOCK)
            b_ref[at, to] = scaled(y_ref[at, to], scale, gm_ref, i).astype(jnp.bfloat16)

        @pl.when(r % 4 == 3)
        def _():
            b_out(r // 4).start()

    @pl.loop(0, n_chunks)
    def _(j):
        y_out(j).wait()
    for i in range(4):
        b_out(i).wait()

    @pl.loop(0, n_pieces)
    def _(n):
        for lane in range(3):
            kv_copy(cp, n, 0, lane, up).wait_send()
    red.given(6)
    red.given(7)
    red.finish()


def attn(x_rows, g_attn, g_mlp, w_q, w_k, w_v, w_o, n_tp, n_cp):
    rows, width = x_rows.shape
    n_heads, hd = w_q.shape[1:]
    bf = jnp.bfloat16
    nq = n_heads * BLOCK
    n = jnp.arange(2 * n_tp, dtype=jnp.int32)
    late = n // n_tp
    cp = lax.axis_index('cp')
    firsts = ((cp * (1 - late) + (2 * n_cp - 1 - cp) * late) * n_tp + n % n_tp) * BLOCK
    points = jnp.concatenate([firsts, jnp.arange(BLOCK, dtype=jnp.int32)]).astype(jnp.float32)
    lane = jnp.arange(hd, dtype=jnp.int32)
    freq = ROPE_THETA ** (-2.0 * (lane % (hd // 2)).astype(jnp.float32) / hd)
    angles = points[:, None] * freq[None, :]
    sign = jnp.where(lane < hd // 2, -1.0, 1.0)
    return pl.pallas_call(
        functools.partial(attn_kernel, n_tp, n_cp, n_heads),
        out_shape=(jax.ShapeDtypeStruct((rows, width), bf),) * 2,
        in_specs=[VM, VM, VM, HBM, HBM, HBM, HBM, VM, VM],
        out_specs=(HBM, HBM),
        scratch_shapes=[
            pltpu.VMEM((4, 2 * rows, width), bf),
            pltpu.VMEM(w_q.shape, bf),
            pltpu.VMEM((width, (n_heads + 2) * hd), bf),
            pltpu.VMEM((2 * n_tp, n_heads, hd, BLOCK), bf),
            pltpu.VMEM((n_cp, n_tp, 2, 2, BLOCK, hd), bf),
            pltpu.VMEM(w_o.shape, bf),
            pltpu.VMEM((rows, width), bf),
            pltpu.VMEM((rows, width), bf),
            pltpu.VMEM((BLOCK, n_heads * hd), bf),
            pltpu.VMEM((hd, nq), bf),
            pltpu.VMEM((KEY_BLOCK, nq), jnp.float32),
            pltpu.VMEM((KEY_BLOCK, nq), jnp.float32),
            pltpu.VMEM((KEY_BLOCK, nq), bf),
            pltpu.VMEM((2, hd, nq), jnp.float32),
            pltpu.VMEM((2, 1, nq), jnp.float32),
            pltpu.VMEM((2, 8, nq), jnp.float32),
            pltpu.VMEM((rows, BLOCK), jnp.float32),
            pltpu.VMEM((2, BLOCK, width), bf),
            *Gather.sems(),
            pltpu.SemaphoreType.DMA((3, 2 * n_tp)),
            pltpu.SemaphoreType.DMA((3, 2 * n_tp)),
            pltpu.SemaphoreType.DMA((4,)),
            pltpu.SemaphoreType.DMA((width // CHUNK + 4,)),
            pltpu.SemaphoreType.REGULAR,
            *rs_sems(width // CHUNK),
        ],
        compiler_params=params(0),
        name='attn',
    )(x_rows, g_attn, g_mlp, w_q, w_k, w_v, w_o, jnp.cos(angles), jnp.sin(angles) * sign)


TILE = 256
COLS = 512
N_W = 2
N_D = 3


def mlp_kernel(n_tp, b_hbm, wg_hbm, wu_hbm, wd_hbm, y_hbm, z_hbm, gath, hid, w, wd, ag_send, ag_recv, w_sem, wd_sem, io_sem, z_sem, txp, rxp, land, *rs):
    red = Reduce(n_tp, b_hbm.shape[1] // CHUNK, txp, lambda o: rxp.at[o], lambda o: land.at[o], *rs)
    ag = Gather(n_tp, lambda half: b_hbm.at[pl.ds(half * BLOCK, BLOCK)], gath, ag_send, ag_recv)
    rows, width = b_hbm.shape
    n_tiles = hid.shape[2] // TILE
    n_cols = width // COLS
    per_chunk = CHUNK // COLS
    own_loads = [pltpu.make_async_copy(ag.src(half), ag.part(0, half), io_sem.at[half]) for half in range(2)]
    for c in own_loads:
        c.start()

    def w_load(g, part):
        src = (wg_hbm, wu_hbm)[part]
        return pltpu.make_async_copy(src.at[:, chunk(g % n_tiles, TILE)], w.at[g % N_W, :, pl.ds(part * TILE, TILE)], w_sem.at[g % N_W, part])

    def w_start(g):
        w_load(g, 0).start()
        w_load(g, 1).start()

    def wd_load(c):
        return pltpu.make_async_copy(wd_hbm.at[:, chunk(c % n_cols, COLS)], wd.at[c % N_D], wd_sem.at[c % N_D])

    with jax.named_scope('mgreet'):
        greet_tp(red)
    ag.start(0)
    ag.start(1)
    for g in range(N_W):
        w_start(g)
    for c in range(N_D):
        wd_load(c).start()

    def gate_up(b):
        where = b - 2 * (b // 3)
        base = b * n_tiles

        @pl.loop(0, n_tiles)
        def _(i):
            w_load(base + i, 0).wait()
            w_load(base + i, 1).wait()
            both = jnp.dot(gath[b], w[(base + i) % N_W], preferred_element_type=jnp.float32)
            gate, up = both[:, :TILE], both[:, TILE:]
            hid[where, :, chunk(i, TILE)] = (gate / (1.0 + jnp.exp(-gate)) * up).astype(jnp.bfloat16)
            w_start(base + i + N_W)

    def down(t, pair, flip):
        with jax.named_scope(f'down{t}'):
            down_pass(t, pair, flip)

    def down_pass(t, pair, flip):
        where = (1, 1, 2, 0)[pair]

        @pl.loop(0, n_cols)
        def _(c):
            n = t * n_cols + c
            wd_load(n).wait()
            part = jnp.dot(hid[where, pl.ds(flip * rows, rows), :], wd[n % N_D], preferred_element_type=jnp.float32)
            wd_load(n + N_D).start()
            j = c // per_chunk
            last = c % per_chunk == per_chunk - 1
            for i in range(2):
                o = 2 * pair + i
                mine = part[i * BLOCK:(i + 1) * BLOCK, :]
                if flip:
                    txp[i, :, chunk(c, COLS)] = mine.astype(jnp.bfloat16)

                    @pl.when(last)
                    def _():
                        red.to_other(o, j).start()
                else:
                    @pl.when(c % per_chunk == 0)
                    def _():
                        red.to_other(o, j).wait_recv()
                    rxp[o, :, chunk(c, COLS)] = (mine + rxp[o, :, chunk(c, COLS)].astype(jnp.float32)).astype(jnp.bfloat16)
                    if pair < 2:
                        @pl.when(last)
                        def _():
                            red.onward(o, j).start()

    def given(pair):
        red.given(2 * pair)
        red.given(2 * pair + 1)

    with jax.named_scope('own'):
        for c in own_loads:
            c.wait()

    @pl.loop(0, 4)
    def _(b):
        for k in range(4):
            @pl.when(b == k)
            def _():
                with jax.named_scope(f'take{k}'):
                    if k == 3:
                        ag.take(k, 0)
                    ag.take(k, 1)
        with jax.named_scope('gate_up'):
            gate_up(b)

        @pl.when(b == 0)
        def _():
            ag.take(1, 0)
            down(0, 3, 1)
            given(3)

        @pl.when(b == 1)
        def _():
            down(1, 1, 1)
            ag.take(2, 0)
            down(2, 1, 0)
            given(1)

    ag.finish()
    y_loads = [pltpu.make_async_copy(y_hbm.at[pl.ds(half * BLOCK, BLOCK)], ag.part(0, half), io_sem.at[half]) for half in range(2)]
    for c in y_loads:
        c.start()
    down(3, 0, 1)
    down(4, 0, 0)
    given(0)
    down(5, 2, 1)
    down(6, 2, 0)
    given(2)
    down(7, 3, 0)
    for i in range(N_D):
        wd_load(UNITS * n_cols + i).wait()
    for i in range(N_W):
        for part in range(2):
            w_load(4 * n_tiles + i, part).wait()

    @pl.loop(0, red.n_chunks)
    def _(j):
        for o in (4, 5):
            red.late(o, j)
            red.onward(o, j).start()
    for c in y_loads:
        c.wait()

    def z_out(j, half):
        return pltpu.make_async_copy(gath.at[0, pl.ds((2 + half) * BLOCK, BLOCK), chunk(j, CHUNK)], z_hbm.at[pl.ds(half * BLOCK, BLOCK), chunk(j, CHUNK)], z_sem.at[half, j])

    @pl.loop(0, red.n_chunks)
    def _(j):
        red.arrive(j)
        for half in range(2):
            @pl.loop(0, 8)
            def _(r):
                at = chunk(r, SUB)
                y = gath[0, chunk(half * 8 + r, SUB), chunk(j, CHUNK)].astype(jnp.float32)
                gath[0, chunk(SUB + half * 8 + r, SUB), chunk(j, CHUNK)] = (y + red.total(half, j, at)).astype(jnp.bfloat16)
            z_out(j, half).start()

    @pl.loop(0, red.n_chunks)
    def _(j):
        for half in range(2):
            z_out(j, half).wait()
    red.finish()


def mlp(b, w_gate, w_up, w_down, y_rows, n_tp):
    bf = jnp.bfloat16
    rows, width = b.shape
    ffn = w_gate.shape[1]
    return pl.pallas_call(
        functools.partial(mlp_kernel, n_tp),
        out_shape=jax.ShapeDtypeStruct((rows, width), bf),
        in_specs=[HBM] * 5,
        out_specs=HBM,
        scratch_shapes=[
            pltpu.VMEM((4, 2 * rows, width), bf),
            pltpu.VMEM((3, 2 * rows, ffn), bf),
            pltpu.VMEM((N_W, width, 2 * TILE), bf),
            pltpu.VMEM((N_D, ffn, COLS), bf),
            *Gather.sems(),
            pltpu.SemaphoreType.DMA((N_W, 2)),
            pltpu.SemaphoreType.DMA((N_D,)),
            pltpu.SemaphoreType.DMA((2,)),
            pltpu.SemaphoreType.DMA((2, width // CHUNK)),
            pltpu.VMEM((2, BLOCK, width), bf),
            pltpu.VMEM((UNITS, BLOCK, width), bf),
            pltpu.VMEM((6, BLOCK, width), bf),
            *rs_sems(width // CHUNK),
        ],
        compiler_params=params(2),
        name='mlp',
    )(b, w_gate, w_up, w_down, y_rows)


def solution(mesh):
    n_cp, n_tp = mesh.shape['cp'], mesh.shape['tp']
    row_spec = P('dp', ('cp', 'tp'))
    cols = P(None, 'tp')

    def local_layer(x, g_attn, w_q, w_k, w_v, w_o, g_mlp, w_gate, w_up, w_down):
        x_rows = x[0]
        width = x_rows.shape[1]
        y, b = attn(x_rows, g_attn.reshape(-1, BLOCK), g_mlp.reshape(-1, BLOCK), w_q, w_k[:, 0], w_v[:, 0], w_o.reshape(-1, width), n_tp, n_cp)
        return mlp(b, w_gate, w_up, w_down, y, n_tp)[None]

    return jax.shard_map(local_layer, mesh=mesh,
                         in_specs=(row_spec, P(), cols, cols, cols, P('tp'), P(), cols, cols, P('tp')),
                         out_specs=row_spec, check_vma=False)
```

```python
import functools

import jax
import jax.numpy as jnp
from jax import lax
from jax.experimental import pallas as pl
from jax.experimental.pallas import tpu as pltpu
from jax.sharding import PartitionSpec as P

NORM_EPS = 1e-5
ROPE_THETA = 500000.0
MESH = pl.DeviceIdType.MESH
VMEM_LIMIT = 67_000_000
LOG2E = 1.4426950408889634
BLOCK = 128
SUB = 16
HIGH = 1024
VM = pl.BlockSpec(memory_space=pltpu.VMEM)
HBM = pl.BlockSpec(memory_space=pl.ANY)


def params(ident):
    return pltpu.CompilerParams(collective_id=ident, has_side_effects=True, vmem_limit_bytes=VMEM_LIMIT)


def remote(src, dst, send_sem, recv_sem, **where):
    return pltpu.make_async_remote_copy(
        src_ref=src, dst_ref=dst, send_sem=send_sem, recv_sem=recv_sem,
        device_id=where, device_id_type=MESH)


def ring(n_tp):
    n_chips = n_tp // 2
    me = lax.axis_index('tp')
    chip, core = me // 2, me % 2
    other = chip * 2 + (1 - core)
    right = ((chip + 1) % n_chips) * 2 + core
    left = ((chip + n_chips - 1) % n_chips) * 2 + core
    return me, chip, core, other, right, left


def greet(barrier, partners, meanwhile=lambda: None):
    for where in partners:
        pl.semaphore_signal(barrier, inc=1, device_id=where, device_id_type=MESH)
    meanwhile()
    pl.semaphore_wait(barrier, len(partners))


def unit_place(o):
    far = (7 - o) // 6
    near = o // 6
    offset = 2 * far + (1 - far - near) * (1 - 2 * (o % 2))
    half = (o % 2 + ((o // 2) % 2) * (1 - o // 4)) % 2
    return offset, half


def pair_of(b):
    mid = ((b + 1) // 2) % 2
    return mid * b + (1 - mid) * (3 - b)


class Chips:
    def __init__(self, n_tp):
        self.n_chips = n_tp // 2
        self.me, self.chip, self.core, self.other, self.right, self.left = ring(n_tp)

    def place(self, o, flip):
        offset, half = unit_place(o)
        return ((self.chip + offset + self.n_chips) % self.n_chips) * 2 + (self.core + flip) % 2, half


class Gather(Chips):
    def __init__(self, n_tp, src, gath, send_sem, recv_sem):
        super().__init__(n_tp)
        self.src, self.gath, self.send_sem, self.recv_sem = src, gath, send_sem, recv_sem

    @staticmethod
    def sems():
        return [pltpu.SemaphoreType.DMA((2, 4, 4)), pltpu.SemaphoreType.DMA((4, 4))]

    def part(self, b, e):
        return self.gath.at[b, pl.ds(e * BLOCK, BLOCK)]

    def copy(self, src, b, e, dst, lane=1):
        return remote(src, self.part(b, e), self.send_sem.at[lane, b, e], self.recv_sem.at[b, e], tp=dst)

    def start(self, half):
        self.copy(self.src(half), 1, 1 - half, (self.right, self.left)[half]).start()
        self.copy(self.src(half), 0, 2 + half, self.other, 0).start()
        if half:
            self.copy(self.src(1), 2, 1, self.right).start()
            self.copy(self.src(0), 2, 0, self.left).start()

    def take(self, b, flip):
        for i in range(2):
            e = 2 * flip + i
            here = self.part(b, e)
            if flip or b:
                self.copy(here, b, e, self.other).wait_recv()
            if b and not flip:
                if b == 1:
                    self.copy(here, 3, 1 - i, (self.left, self.right)[i]).start()
                self.copy(here, b, 2 + i, self.other, 0).start()

    def finish(self):
        for i in range(2):
            for b in range(4):
                self.copy(self.src(0), b, 2 + i, self.other, 0).wait_send()
                if b:
                    self.copy(self.src(0), b, i, self.other).wait_send()


def chunk(j, size):
    return pl.ds(j * size if isinstance(j, int) else pl.multiple_of(j * size, size), size)


KEY_BLOCK = 512
HIDDEN = -1e30
EXP_ROWS = 64


class Attend:
    def __init__(self, q_tile, kv_ref, n_cp, n_tp, buffers, p_ref, acc_ref, m_ref, l_ref):
        self.q_tile, self.kv_ref, self.n_cp, self.n_tp = q_tile, kv_ref, n_cp, n_tp
        self.buffers, self.p_ref, self.acc_ref, self.m_ref, self.l_ref = buffers, p_ref, acc_ref, m_ref, l_ref
        self.c = LOG2E * q_tile.shape[0] ** -0.5

    def reset(self):
        self.acc_ref[...] = jnp.zeros_like(self.acc_ref)
        self.m_ref[...] = jnp.full(self.m_ref.shape, HIDDEN, jnp.float32)
        self.l_ref[...] = jnp.zeros_like(self.l_ref)

    def place(self, n):
        per_piece = self.n_tp * BLOCK // KEY_BLOCK
        piece = n // per_piece
        late = piece // self.n_cp
        block = piece * (1 - late) + (2 * self.n_cp - 1 - piece) * late
        return block, (n % per_piece) * (KEY_BLOCK // 256) + late * (self.n_tp // 2)

    def scores(self, n, dst, shift=None):
        j, t = self.place(n)
        q = self.q_tile[...]
        keys = self.kv_ref[j, pl.ds(t, KEY_BLOCK // 256), :, 0].reshape(KEY_BLOCK, q.shape[0])
        s = jnp.dot(keys, q, preferred_element_type=jnp.float32)
        if shift is not None:
            row = lax.broadcasted_iota(jnp.int32, s.shape, 1) % BLOCK
            s = jnp.where(lax.broadcasted_iota(jnp.int32, s.shape, 0) <= row + shift, s, HIDDEN)
        dst[0][...] = s
        dst[1][...] = jnp.max(s.reshape(-1, 8, s.shape[1]), axis=0)

    def process(self, n, src):
        j, t = self.place(n)
        s_ref, m8 = src
        m = self.m_ref[...]
        m_new = jnp.maximum(m, jnp.max(m8[...], axis=0, keepdims=True))
        self.m_ref[...] = m_new
        alpha = jnp.exp2((m - m_new) * self.c)
        mc = m_new * self.c
        l8 = self.l_ref[...] * alpha
        for r in range(0, KEY_BLOCK, EXP_ROWS):
            p = jnp.exp2(s_ref[r:r + EXP_ROWS, :] * self.c - mc)
            l8 = l8 + jnp.sum(p.reshape(-1, *m8.shape), axis=0)
            self.p_ref[r:r + EXP_ROWS, :] = p.astype(jnp.bfloat16)
        self.l_ref[...] = l8
        v_t = jnp.concatenate([self.kv_ref[j, t + i // 2, i % 2, 1] for i in range(KEY_BLOCK // BLOCK)], axis=1)
        self.acc_ref[...] = self.acc_ref[...] * alpha + jnp.dot(v_t, self.p_ref[...], preferred_element_type=jnp.float32)

    def sweep(self, start, shift, count, base, step):
        sa, sb = self.buffers

        self.scores(start, sa, shift)

        @pl.loop(0, count // 2)
        def _(k):
            fresh = 1 - (k + HIGH - 1) // HIGH
            self.scores(base + step * 2 * k, sb)
            self.process(fresh * start + (1 - fresh) * (base + step * (2 * k - 1)), sa)
            self.scores(base + step * (2 * k + 1), sa)
            self.process(base + step * 2 * k, sb)

        even = count // 2 * 2
        fresh = 1 - (even + HIGH - 1) // HIGH
        held = fresh * start + (1 - fresh) * (base + step * (even - 1))

        @pl.when(count % 2 == 1)
        def _():
            self.scores(base + step * even, sb)
            self.process(held, sa)
            self.process(base + step * even, sb)

        @pl.when(count % 2 == 0)
        def _():
            self.process(held, sa)

    def sweep_if_any(self, count, base, step):
        @pl.when(count > 0)
        def _():
            self.sweep(base, None, count - 1, base + step, step)

    def result(self):
        return self.acc_ref[...] / jnp.sum(self.l_ref[...], axis=0, keepdims=True)


CHUNK = 1024
UNITS = 8


class Reduce(Chips):
    def __init__(self, n_tp, n_chunks, txp, rxp, land, peer_sem, ring_sem):
        super().__init__(n_tp)
        self.n_chunks = n_chunks
        self.txp = lambda o, j: txp.at[o % 2, :, chunk(j, CHUNK)]
        self.rxp = lambda o, j: rxp(o).at[:, chunk(j, CHUNK)]
        self.land = lambda o, j: land(o).at[:, chunk(j, CHUNK)]
        self.peer_sem, self.ring_sem = peer_sem, ring_sem

    def to_other(self, o, j):
        return remote(self.txp(o, j), self.rxp(o, j), self.peer_sem.at[0, o, j], self.peer_sem.at[1, o, j], tp=self.other)

    def onward(self, o, j):
        odd = o % 2
        return remote(self.rxp(o, j), self.land(o, j), self.ring_sem.at[0, o, j], self.ring_sem.at[1, o, j],
                      tp=self.right * (1 - odd) + self.left * odd)

    def give(self, o, j, value):
        self.txp(o, j)[...] = value.astype(jnp.bfloat16)
        self.to_other(o, j).start()

    def given(self, o):
        @pl.loop(0, self.n_chunks)
        def _(j):
            self.to_other(o, j).wait_send()

    def add(self, o, j, value):
        self.rxp(o, j)[...] = (value + self.rxp(o, j)[...].astype(jnp.float32)).astype(jnp.bfloat16)

    def late(self, o, j):
        self.onward(o - 4, j).wait_recv()
        self.add(o, j, self.land(o - 4, j)[...].astype(jnp.float32))

    def total(self, half, j, rows):
        parts = self.rxp(6 + half, j), self.land((4, 2)[half], j), self.land((3, 5)[half], j)
        return sum(p[rows, :].astype(jnp.float32) for p in parts).astype(jnp.bfloat16).astype(jnp.float32)

    def arrive(self, j):
        for o in range(2, 6):
            self.onward(o, j).wait_recv()

    def sent(self, j):
        for o in range(6):
            self.onward(o, j).wait_send()


def rs_sems(n_chunks):
    return [pltpu.SemaphoreType.DMA((2, UNITS, n_chunks)), pltpu.SemaphoreType.DMA((2, 6, n_chunks))]


def greet_tp(r):
    greet(pltpu.get_barrier_semaphore(), [{'tp': r.other}, {'tp': r.right}, {'tp': r.left}])


def scaled(ref, scale, gain_ref, lane):
    return ref.astype(jnp.float32) * scale * gain_ref[lane:lane + 1, :].astype(jnp.float32)


def attn_kernel(n_tp, n_cp, n_heads, x_hbm, ga_ref, gm_ref, wq_hbm, wk_hbm, wv_hbm, wo_hbm, cos_ref, sin_ref, y_hbm, b_hbm,
                gath, x_ref, wraw, wcat, q_ref, kv_ref, wo, y_ref, b_ref, a_tile, q_tile, sa, sb, m8, p, acc, m, l, sq, txp,
                ag_send, ag_recv, kv_send, kv_recv, x_sem, local, out_sem, free, *rs):
    ag = Gather(n_tp, lambda half: gath.at[0, pl.ds(half * BLOCK, BLOCK)], gath, ag_send, ag_recv)
    width = gath.shape[2]
    n_chunks = width // CHUNK
    unit = lambda o: gath.at[o // 4, chunk(o % 4, BLOCK)]
    red = Reduce(n_tp, n_chunks, txp, unit, lambda o: unit(o + UNITS), *rs)
    cp = lax.axis_index('cp')
    up, down = (cp + 1) % n_cp, (cp + n_cp - 1) % n_cp
    hd = BLOCK
    qw = n_heads * hd
    n_pieces = q_ref.shape[0]
    n_steps = n_pieces // 2
    lanes = range(width // BLOCK)
    tp_partners = [{'tp': ag.other}, {'tp': ag.right}, {'tp': ag.left}]

    def x_load(half):
        at = pl.ds(half * BLOCK, BLOCK)
        return pltpu.make_async_copy(x_hbm.at[at], x_ref.at[at], x_sem.at[half])

    x_load(0).start()
    x_load(1).start()
    loads = [
        pltpu.make_async_copy(wq_hbm, wraw, local.at[0]),
        pltpu.make_async_copy(wk_hbm, wcat.at[:, pl.ds(qw, hd)], local.at[1]),
        pltpu.make_async_copy(wv_hbm, wcat.at[:, pl.ds(qw + hd, hd)], local.at[2]),
        pltpu.make_async_copy(wo_hbm, wo, local.at[3]),
    ]

    def norm(half):
        x_load(half).wait()

        @pl.loop(0, 8)
        def _(r):
            x = x_ref[chunk(half * 8 + r, SUB), :].astype(jnp.float32)
            scale = lax.rsqrt(jnp.sum(x * x, axis=-1, keepdims=True) / width + NORM_EPS)
            for i in lanes:
                at = slice(i * BLOCK, (i + 1) * BLOCK)
                gath[0, chunk(half * 8 + r, SUB), at] = scaled(x[:, at], scale, ga_ref, i).astype(jnp.bfloat16)

    greet(pltpu.get_barrier_semaphore(), [*tp_partners, {'cp': up}, {'cp': down}], lambda: norm(0))
    ag.start(0)
    norm(1)
    ag.start(1)
    for c in loads:
        c.start()

    def place(n):
        return ag.place(2 * pair_of(n // 4) + n % 2, (n // 2) % 2)

    def kv_copy(where, n, kind, lane, dst):
        slot, half = place(n)
        piece = kv_ref.at[where, slot, half]
        return remote(piece, piece, kv_send.at[lane, n], kv_recv.at[kind, n], cp=dst)

    def kv_forward(n):
        kv_copy(down, n, 0, 0, up).wait_recv()
        kv_copy(up, n, 1, 0, up).wait_recv()
        odd = n % 2
        kv_copy(down * (1 - odd) + up * odd, n, 2, 2, up * (1 - odd) + down * odd).start()

    for c in loads:
        c.wait()

    with jax.named_scope('wcat'):
        @pl.loop(0, wraw.shape[0] // BLOCK)
        def _(i):
            block = wraw[chunk(i, BLOCK)]
            for h in range(n_heads):
                wcat[chunk(i, BLOCK), h * hd:(h + 1) * hd] = block[:, h, :]

    def kv_far(begin, end):
        @pl.loop(begin, end)
        def _(n):
            kv_copy((cp + 2) % n_cp, n, 2, 0, up).wait_recv()

    def order(i):
        o = (1 - i // 4) * ((i + 2) % 4) + i // 4 * i
        swap = 1 - (red.chip + 1) // 2 % 2
        return o + swap * (1 - 2 * (o % 2))

    def tile(o, flip):
        slot, half = red.place(o, flip)
        late = slot // (n_tp // 2)
        first = ((cp * (1 - late) + (2 * n_cp - 1 - cp) * late) * n_tp + slot % (n_tp // 2) * 2 + half) * BLOCK
        for h in range(n_heads):
            q_tile[:, h * BLOCK:(h + 1) * BLOCK] = q_ref[4 * pair_of(o // 2) + 2 * flip + o % 2, h]
        work = Attend(q_tile, kv_ref, n_cp, n_tp, ((sa, m8.at[0]), (sb, m8.at[1])), p, acc.at[flip], m.at[flip], l.at[flip])
        return work, first // KEY_BLOCK, first % KEY_BLOCK

    def far_blocks(n_full):
        half = red.n_chips // 2
        per_half = n_cp * half
        far_late = 1 - red.chip // half
        early = n_full - (n_full // per_half) * (n_full - per_half)
        late = n_full - early
        mixed = far_late * late + (1 - far_late) * early
        at, parity = far_late * per_half, red.chip % half
        return (((mixed - parity + 1) // 2, at + parity, 2),
                ((n_full - mixed, per_half - at, 1), ((mixed + parity) // 2, at + 1 - parity, 2)))

    fine = pl.ds(cos_ref.shape[0] - BLOCK, BLOCK)

    @pl.loop(0, n_steps)
    def _(s):
        for k in range(n_steps):
            @pl.when(s == k)
            def _():
                with jax.named_scope(f'take{k}'):
                    ag.take(k // 2, k % 2)
        product = jnp.dot(gath[s // 2, chunk(s % 2, 256), :], wcat[...], preferred_element_type=jnp.float32)
        for i in range(2):
            n = 2 * s + i
            slot, half = place(n)
            part = product[i * BLOCK:(i + 1) * BLOCK, :]
            coarse = pl.ds(slot * 2 + half, 1)
            cos0, sin0 = cos_ref[coarse, :], sin_ref[coarse, :]
            cos = cos0 * cos_ref[fine, :] - sin0 * sin_ref[fine, :]
            sin = sin0 * cos_ref[fine, :] + cos0 * sin_ref[fine, :]

            def rope(t):
                t = t.astype(jnp.bfloat16).astype(jnp.float32)
                return (t * cos + pltpu.roll(t, hd // 2, 1) * sin).astype(jnp.bfloat16)

            kv_ref[cp, slot, half, 0] = rope(part[:, qw:qw + hd])
            kv_ref[cp, slot, half, 1] = part[:, qw + hd:].T.astype(jnp.bfloat16)
            for h in range(n_heads):
                q_ref[n, h] = rope(part[:, h * hd:(h + 1) * hd]).astype(jnp.float32).T.astype(jnp.bfloat16)
        for i in range(2):
            kv_copy(cp, 2 * s + i, 0, 0, up).start()
            kv_copy(cp, 2 * s + i, 1, 1, down).start()

        @pl.when((s >= 1) & (s != n_steps - 2))
        def _():
            kv_forward(2 * s - 2)
            kv_forward(2 * s - 1)

        @pl.when(s == n_steps - 3)
        def _():
            with jax.named_scope('early'):
                kv_forward(2 * s)
                kv_forward(2 * s + 1)
                kv_far(0, n_pieces - 4)
                o = order(0)
                for flip in (1, 0):
                    work, n_full, _ = tile(o, flip)
                    far, others = far_blocks(n_full)
                    work.reset()
                    for blocks in others:
                        work.sweep_if_any(*blocks)

    ag.finish()
    for where in tp_partners:
        pl.semaphore_signal(free, inc=1, device_id=where, device_id_type=MESH)
    with jax.named_scope('kvtail'):
        for n in range(n_pieces - 2, n_pieces):
            kv_forward(n)

        kv_far(n_pieces - 4, n_pieces)
    pl.semaphore_wait(free, len(tp_partners))

    @pl.loop(0, 2 * UNITS)
    def _(u):
        o = order(u // 2)
        flip = 1 - u % 2
        work, n_full, shift = tile(o, flip)
        begun = 1 - (u + 2 * UNITS - 2) // (2 * UNITS)
        far, _ = far_blocks(n_full)

        @pl.when(begun == 0)
        def _():
            work.reset()
        with jax.named_scope('attend'):
            work.sweep(n_full, shift, *(begun * f + (1 - begun) * w for f, w in zip(far, (n_full, 0, 1))))
        out = work.result()
        for h in range(n_heads):
            a_tile[:, h * hd:(h + 1) * hd] = out[:, h * BLOCK:(h + 1) * BLOCK].T.astype(jnp.bfloat16)

        def product(j):
            return jnp.dot(a_tile[...], wo[:, chunk(j, CHUNK)], preferred_element_type=jnp.float32)

        @pl.when(flip == 1)
        def _():
            @pl.when(u >= 4)
            def _():
                red.given(order(u // 2 - 2))

            with jax.named_scope('give'):
                for j in range(n_chunks):
                    red.give(o, j, product(j))

        @pl.when(flip == 0)
        def _():
            with jax.named_scope('keep'):
                for j in range(n_chunks):
                    red.to_other(o, j).wait_recv()
                for j in range(n_chunks):
                    red.add(o, j, product(j))

                @pl.when(o < 4)
                def _():
                    for j in range(n_chunks):
                        red.onward(o, j).start()

            @pl.when(u // 2 == 5 + red.chip // (red.n_chips // 2))
            def _():
                with jax.named_scope('late'):
                    @pl.loop(0, n_chunks)
                    def _(j):
                        for o in (4, 5):
                            red.late(o, j)
                            red.onward(o, j).start()

    sq[...] = jnp.zeros_like(sq)

    @pl.loop(0, n_pieces)
    def _(n):
        for lane in range(3):
            kv_copy(cp, n, 0, lane, up).wait_send()
    red.given(6)
    red.given(7)

    def y_out(j):
        return pltpu.make_async_copy(y_ref.at[:, chunk(j, CHUNK)], y_hbm.at[:, chunk(j, CHUNK)], out_sem.at[j])

    def b_out(i):
        return pltpu.make_async_copy(b_ref.at[chunk(i, 64)], b_hbm.at[chunk(i, 64)], out_sem.at[n_chunks + i])

    @pl.loop(0, n_chunks)
    def _(j):
        with jax.named_scope('arrive'):
            red.arrive(j)
        for half in range(2):
            @pl.loop(0, 8)
            def _(r):
                at = chunk(half * 8 + r, SUB)
                y = (x_ref[at, chunk(j, CHUNK)].astype(jnp.float32) + red.total(half, j, chunk(r, SUB))).astype(jnp.bfloat16)
                y_ref[at, chunk(j, CHUNK)] = y
                yf = y.astype(jnp.float32)
                y2 = yf * yf
                sq[at, :] += sum(y2[:, i * BLOCK:(i + 1) * BLOCK] for i in range(CHUNK // BLOCK))
        y_out(j).start()
        red.sent(j)

    sq[...] = jnp.broadcast_to(lax.rsqrt(jnp.sum(sq[...], axis=-1, keepdims=True) / width + NORM_EPS), sq.shape)

    @pl.loop(0, SUB)
    def _(r):
        at = chunk(r, SUB)
        for i in lanes:
            to = slice(i * BLOCK, (i + 1) * BLOCK)
            b_ref[at, to] = scaled(y_ref[at, to], sq[at, :], gm_ref, i).astype(jnp.bfloat16)

        @pl.when(r % 4 == 3)
        def _():
            b_out(r // 4).start()

    @pl.loop(0, n_chunks)
    def _(j):
        y_out(j).wait()
    for i in range(4):
        b_out(i).wait()


def attn(x_rows, g_attn, g_mlp, w_q, w_k, w_v, w_o, n_tp, n_cp):
    rows, width = x_rows.shape
    n_heads, hd = w_q.shape[1:]
    bf = jnp.bfloat16
    nq = n_heads * BLOCK
    n = jnp.arange(2 * n_tp, dtype=jnp.int32)
    late = n // n_tp
    cp = lax.axis_index('cp')
    firsts = ((cp * (1 - late) + (2 * n_cp - 1 - cp) * late) * n_tp + n % n_tp) * BLOCK
    points = jnp.concatenate([firsts, jnp.arange(BLOCK, dtype=jnp.int32)]).astype(jnp.float32)
    lane = jnp.arange(hd, dtype=jnp.int32)
    freq = ROPE_THETA ** (-2.0 * (lane % (hd // 2)).astype(jnp.float32) / hd)
    angles = points[:, None] * freq[None, :]
    sign = jnp.where(lane < hd // 2, -1.0, 1.0)
    return pl.pallas_call(
        functools.partial(attn_kernel, n_tp, n_cp, n_heads),
        out_shape=(jax.ShapeDtypeStruct((rows, width), bf),) * 2,
        in_specs=[HBM, VM, VM, HBM, HBM, HBM, HBM, VM, VM],
        out_specs=(HBM, HBM),
        scratch_shapes=[
            pltpu.VMEM((4, 2 * rows, width), bf),
            pltpu.VMEM((rows, width), bf),
            pltpu.VMEM(w_q.shape, bf),
            pltpu.VMEM((width, (n_heads + 2) * hd), bf),
            pltpu.VMEM((2 * n_tp, n_heads, hd, BLOCK), bf),
            pltpu.VMEM((n_cp, n_tp, 2, 2, BLOCK, hd), bf),
            pltpu.VMEM(w_o.shape, bf),
            pltpu.VMEM((rows, width), bf),
            pltpu.VMEM((rows, width), bf),
            pltpu.VMEM((BLOCK, n_heads * hd), bf),
            pltpu.VMEM((hd, nq), bf),
            pltpu.VMEM((KEY_BLOCK, nq), jnp.float32),
            pltpu.VMEM((KEY_BLOCK, nq), jnp.float32),
            pltpu.VMEM((2, 8, nq), jnp.float32),
            pltpu.VMEM((KEY_BLOCK, nq), bf),
            pltpu.VMEM((2, hd, nq), jnp.float32),
            pltpu.VMEM((2, 1, nq), jnp.float32),
            pltpu.VMEM((2, 8, nq), jnp.float32),
            pltpu.VMEM((rows, BLOCK), jnp.float32),
            pltpu.VMEM((2, BLOCK, width), bf),
            *Gather.sems(),
            pltpu.SemaphoreType.DMA((3, 2 * n_tp)),
            pltpu.SemaphoreType.DMA((3, 2 * n_tp)),
            pltpu.SemaphoreType.DMA((2,)),
            pltpu.SemaphoreType.DMA((4,)),
            pltpu.SemaphoreType.DMA((width // CHUNK + 4,)),
            pltpu.SemaphoreType.REGULAR,
            *rs_sems(width // CHUNK),
        ],
        compiler_params=params(0),
        name='attn',
    )(x_rows, g_attn, g_mlp, w_q, w_k, w_v, w_o, jnp.cos(angles), jnp.sin(angles) * sign)


PLACES = (1, 1, 2, 0)
TILE = 256
COLS = 512
N_W = 2
N_D = 3


def mlp_kernel(n_tp, b_hbm, wg_hbm, wu_hbm, wd_hbm, y_hbm, z_hbm, gath, hid, w, wd, ag_send, ag_recv, w_sem, wd_sem, io_sem, z_sem, mine, txp, rxp, land, *rs):
    red = Reduce(n_tp, b_hbm.shape[1] // CHUNK, txp, lambda o: rxp.at[o], lambda o: land.at[o], *rs)
    ag = Gather(n_tp, lambda half: b_hbm.at[pl.ds(half * BLOCK, BLOCK)], gath, ag_send, ag_recv)
    rows, width = b_hbm.shape
    n_tiles = hid.shape[2] // TILE
    n_cols = width // COLS
    per_chunk = CHUNK // COLS
    own_loads = [pltpu.make_async_copy(ag.src(half), ag.part(0, half), io_sem.at[half]) for half in range(2)]
    for c in own_loads:
        c.start()

    def w_load(g, part):
        src = (wg_hbm, wu_hbm)[part]
        return pltpu.make_async_copy(src.at[:, chunk(g % n_tiles, TILE)], w.at[g % N_W, :, pl.ds(part * TILE, TILE)], w_sem.at[g % N_W, part])

    def w_start(g):
        w_load(g, 0).start()
        w_load(g, 1).start()

    def wd_load(c):
        return pltpu.make_async_copy(wd_hbm.at[:, chunk(c % n_cols, COLS)], wd.at[c % N_D], wd_sem.at[c % N_D])

    with jax.named_scope('mgreet'):
        greet_tp(red)
    ag.start(0)
    ag.start(1)
    for g in range(N_W):
        w_start(g)
    for c in range(N_D):
        wd_load(c).start()

    def gate_up(b):
        where = b - 2 * (b // 3)
        base = b * n_tiles

        @pl.loop(0, n_tiles)
        def _(i):
            w_load(base + i, 0).wait()
            w_load(base + i, 1).wait()
            both = jnp.dot(gath[b], w[(base + i) % N_W], preferred_element_type=jnp.float32)
            gate, up = both[:, :TILE], both[:, TILE:]
            hid[where, :, chunk(i, TILE)] = (gate / (1.0 + jnp.exp(-gate)) * up).astype(jnp.bfloat16)
            w_start(base + i + N_W)

    def down(t, pair, flip):
        where = PLACES[pair]

        @pl.loop(0, n_cols)
        def _(c):
            n = t * n_cols + c
            wd_load(n).wait()
            part = jnp.dot(hid[where, pl.ds(flip * rows, rows), :], wd[n % N_D], preferred_element_type=jnp.float32)
            wd_load(n + N_D).start()
            j = c // per_chunk
            last = c % per_chunk == per_chunk - 1
            for i in range(2):
                o = 2 * pair + i
                mine = part[i * BLOCK:(i + 1) * BLOCK, :]
                if flip:
                    txp[i, :, chunk(c, COLS)] = mine.astype(jnp.bfloat16)

                    @pl.when(last)
                    def _():
                        red.to_other(o, j).start()
                else:
                    @pl.when(c % per_chunk == 0)
                    def _():
                        red.to_other(o, j).wait_recv()
                    rxp[o, :, chunk(c, COLS)] = (mine + rxp[o, :, chunk(c, COLS)].astype(jnp.float32)).astype(jnp.bfloat16)
                    if pair < 2:
                        @pl.when(last)
                        def _():
                            red.onward(o, j).start()

    def down_both(t, pair):
        where = PLACES[pair]

        def combine(j):
            for i in range(2):
                o = 2 * pair + i
                red.to_other(o, j).wait_recv()
                red.add(o, j, mine[2 * (j % 2) + i].astype(jnp.float32))
                if pair < 2:
                    red.onward(o, j).start()

        @pl.loop(0, n_cols)
        def _(c):
            n = t * n_cols + c
            wd_load(n).wait()
            part = jnp.dot(hid[where], wd[n % N_D], preferred_element_type=jnp.float32)
            wd_load(n + N_D).start()
            j = c // per_chunk
            for i in range(2):
                mine[2 * (j % 2) + i, :, chunk(c % per_chunk, COLS)] = part[i * BLOCK:(i + 1) * BLOCK, :].astype(jnp.bfloat16)
                txp[i, :, chunk(c, COLS)] = part[rows + i * BLOCK:rows + (i + 1) * BLOCK, :].astype(jnp.bfloat16)

            @pl.when(c % per_chunk == per_chunk - 1)
            def _():
                for i in range(2):
                    red.to_other(2 * pair + i, j).start()

                @pl.when(j > 0)
                def _():
                    combine(j - 1)
        combine(red.n_chunks - 1)

    def given(pair):
        red.given(2 * pair)
        red.given(2 * pair + 1)

    with jax.named_scope('own'):
        for c in own_loads:
            c.wait()

    @pl.loop(0, 4)
    def _(b):
        for k in range(4):
            @pl.when(b == k)
            def _():
                with jax.named_scope(f'take{k}'):
                    ag.take(k, 1)
        with jax.named_scope('gate_up'):
            gate_up(b)

        @pl.when(b == 0)
        def _():
            down(0, 3, 1)
            ag.take(1, 0)
            given(3)

        @pl.when(b == 1)
        def _():
            ag.take(2, 0)
            down(1, 1, 1)

        @pl.when(b == 2)
        def _():
            ag.take(3, 0)
            down(2, 1, 0)
            given(1)

    ag.finish()
    y_loads = [pltpu.make_async_copy(y_hbm.at[pl.ds(half * BLOCK, BLOCK)], ag.part(0, half), io_sem.at[half]) for half in range(2)]
    for c in y_loads:
        c.start()
    down_both(3, 0)
    given(0)
    down_both(4, 2)
    given(2)
    down(5, 3, 0)
    for i in range(N_D):
        wd_load(6 * n_cols + i).wait()
    for i in range(N_W):
        for part in range(2):
            w_load(4 * n_tiles + i, part).wait()

    @pl.loop(0, red.n_chunks)
    def _(j):
        for o in (4, 5):
            red.late(o, j)
            red.onward(o, j).start()
    for c in y_loads:
        c.wait()

    def z_out(j, half):
        return pltpu.make_async_copy(gath.at[0, pl.ds((2 + half) * BLOCK, BLOCK), chunk(j, CHUNK)], z_hbm.at[pl.ds(half * BLOCK, BLOCK), chunk(j, CHUNK)], z_sem.at[half, j])

    @pl.loop(0, red.n_chunks)
    def _(j):
        red.arrive(j)
        for half in range(2):
            @pl.loop(0, 8)
            def _(r):
                at = chunk(r, SUB)
                y = gath[0, chunk(half * 8 + r, SUB), chunk(j, CHUNK)].astype(jnp.float32)
                gath[0, chunk(SUB + half * 8 + r, SUB), chunk(j, CHUNK)] = (y + red.total(half, j, at)).astype(jnp.bfloat16)
            z_out(j, half).start()
        red.sent(j)

    @pl.loop(0, red.n_chunks)
    def _(j):
        for half in range(2):
            z_out(j, half).wait()


def mlp(b, w_gate, w_up, w_down, y_rows, n_tp):
    bf = jnp.bfloat16
    rows, width = b.shape
    ffn = w_gate.shape[1]
    return pl.pallas_call(
        functools.partial(mlp_kernel, n_tp),
        out_shape=jax.ShapeDtypeStruct((rows, width), bf),
        in_specs=[HBM] * 5,
        out_specs=HBM,
        scratch_shapes=[
            pltpu.VMEM((4, 2 * rows, width), bf),
            pltpu.VMEM((3, 2 * rows, ffn), bf),
            pltpu.VMEM((N_W, width, 2 * TILE), bf),
            pltpu.VMEM((N_D, ffn, COLS), bf),
            *Gather.sems(),
            pltpu.SemaphoreType.DMA((N_W, 2)),
            pltpu.SemaphoreType.DMA((N_D,)),
            pltpu.SemaphoreType.DMA((2,)),
            pltpu.SemaphoreType.DMA((2, width // CHUNK)),
            pltpu.VMEM((4, BLOCK, CHUNK), bf),
            pltpu.VMEM((2, BLOCK, width), bf),
            pltpu.VMEM((UNITS, BLOCK, width), bf),
            pltpu.VMEM((6, BLOCK, width), bf),
            *rs_sems(width // CHUNK),
        ],
        compiler_params=params(2),
        name='mlp',
    )(b, w_gate, w_up, w_down, y_rows)


def solution(mesh):
    n_cp, n_tp = mesh.shape['cp'], mesh.shape['tp']
    row_spec = P('dp', ('cp', 'tp'))
    cols = P(None, 'tp')

    def local_layer(x, g_attn, w_q, w_k, w_v, w_o, g_mlp, w_gate, w_up, w_down):
        x_rows = x[0]
        width = x_rows.shape[1]
        y, b = attn(x_rows, g_attn.reshape(-1, BLOCK), g_mlp.reshape(-1, BLOCK), w_q, w_k[:, 0], w_v[:, 0], w_o.reshape(-1, width), n_tp, n_cp)
        return mlp(b, w_gate, w_up, w_down, y, n_tp)[None]

    return jax.shard_map(local_layer, mesh=mesh,
                         in_specs=(row_spec, P(), cols, cols, cols, P('tp'), P(), cols, cols, P('tp')),
                         out_specs=row_spec, check_vma=False)
```
